8 devices in a mesh: terms: 8 (over z, y, x, core).
Axes of the slice: x: 2, y: 2, z: 1, core: 2. Of those that a mesh axis runs over, the one named last changes fastest.
Arguments:
- psi_init: float32 [896, 4, 4, 896], replicated
- left_env: bfloat16 [16, 896, 896], P('terms')
- op_pair: bfloat16 [16, 16, 16], P('terms')
- right_env: bfloat16 [16, 896, 896], P('terms')
Outputs:
- output 1: float32 [7, 896, 4, 4, 896], P(None, 'terms')
- output 2: float32 [6], replicated
- output 3: float32 [6], replicated
All inputs are finite; a program needn't handle non-finite values.
Results may differ from the reference program's by a relative error of at most 0.0161663.
Values are sent between devices in bfloat16 or wider.
A program may use at most 1 GiB of HBM per device.

```python
import jax
import jax.numpy as jnp
from jax import lax

BOND = 896
PHYS = 4
TERMS = 16
KRYLOV_STEPS = 6


def symmetric_stack(key_in, count, size):
    gauss_draws = jax.random.normal(key_in, (count, size, size), jnp.float32)
    return (gauss_draws + jnp.swapaxes(gauss_draws, 1, 2)) * (0.5 * (2.0 * size) ** -0.5)


def setup_inputs(seed: int = 0) -> dict:
    root_key = jax.random.key(seed)
    key_psi, key_left, key_pair, key_right, key_shift = jax.random.split(root_key, 5)
    pair_dim = PHYS * PHYS
    shifts = 0.5 * jax.random.normal(key_shift, (3, TERMS), jnp.float32)
    eye_bond = jnp.eye(BOND, dtype=jnp.float32)
    eye_pair = jnp.eye(pair_dim, dtype=jnp.float32)
    term_scale = 2.0 * TERMS ** -0.5
    psi_init = jax.random.normal(key_psi, (BOND, PHYS, PHYS, BOND), jnp.float32)
    left_env = term_scale * (symmetric_stack(key_left, TERMS, BOND) + shifts[0][:, None, None] * eye_bond)
    op_pair = symmetric_stack(key_pair, TERMS, pair_dim) + shifts[1][:, None, None] * eye_pair
    right_env = symmetric_stack(key_right, TERMS, BOND) + shifts[2][:, None, None] * eye_bond
    return {'psi_init': psi_init, 'left_env': left_env.astype(jnp.bfloat16), 'op_pair': op_pair.astype(jnp.bfloat16), 'right_env': right_env.astype(jnp.bfloat16)}


def reference(psi_init, left_env, op_pair, right_env):
    pair_dim = PHYS * PHYS
    elem_count = BOND * pair_dim * BOND

    def apply_terms(vector):
        vector_low = vector.astype(jnp.bfloat16).reshape(BOND * pair_dim, BOND)

        def one_term(sigma_sum, term_mats):
            left_mat, pair_mat, right_mat = term_mats
            y_part = jnp.dot(vector_low, right_mat.T, preferred_element_type=jnp.float32)
            y_part = y_part.astype(jnp.bfloat16).reshape(BOND, pair_dim, BOND)
            z_part = jnp.einsum('qp,apb->aqb', pair_mat.astype(jnp.float32), y_part.astype(jnp.float32))
            z_part = z_part.astype(jnp.bfloat16).reshape(BOND, pair_dim * BOND)
            term_out = jnp.dot(left_mat, z_part, preferred_element_type=jnp.float32)
            return sigma_sum + term_out.reshape(BOND, pair_dim, BOND), None

        sigma_sum, _ = lax.scan(one_term, jnp.zeros((BOND, pair_dim, BOND), jnp.float32), (left_env, op_pair, right_env))
        return sigma_sum

    vector = psi_init.reshape(BOND, pair_dim, BOND)
    vector = vector / jnp.sqrt(jnp.sum(vector * vector) / elem_count)
    vectors = [vector]
    alphas = []
    betas = []
    prev_vector = vector
    for step_idx in range(KRYLOV_STEPS):
        sigma_sum = apply_terms(vector)
        alpha_val = jnp.sum(sigma_sum * vector) / elem_count
        residual = sigma_sum - alpha_val * vector
        if step_idx > 0:
            residual = residual - betas[-1] * prev_vector
        beta_val = jnp.sqrt(jnp.sum(residual * residual) / elem_count)
        prev_vector = vector
        vector = residual / beta_val
        vectors.append(vector)
        alphas.append(alpha_val)
        betas.append(beta_val)
    krylov_vectors = jnp.stack(vectors).reshape(KRYLOV_STEPS + 1, BOND, PHYS, PHYS, BOND)
    return krylov_vectors, jnp.stack(alphas), jnp.stack(betas)
```

```python
import jax
import jax.numpy as jnp
from jax import lax
from jax.experimental import pallas as pl
from jax.experimental.pallas import tpu as pltpu
from jax.sharding import PartitionSpec as P

STEPS = 6
BOND = 896
NP = 16
TERMS = 16
NDEV = 8
ROWS = BOND // NDEV
LANES = 128
NCH = BOND // LANES
KG = 4
NKG = TERMS // KG
UNITS = NCH * NKG
SLAB = NP * ROWS
ELEMS = BOND * NP * BOND
MESH = pl.DeviceIdType.MESH
NS = ((0, 512), (512, 1024), (1024, 1536), (1536, 1792))


def kernel(v0_h, slab_h, left_h, kron_h, right_h, vout_h, ab_ref,
           vbuf, left, kron, rblk, sig, ubuf, zbuf, vecs, mine, exch,
           load_sem, v0_sem, r_sem, out_sem, send_sem, recv_sem, xs_sem, xr_sem):
    me = lax.axis_index('terms')
    core = lax.rem(me, 2)
    xpos = lax.rem(lax.div(me, 2), 2)
    ypos = lax.div(me, 4)
    sib = me + 1 - 2 * core
    xn = me + 2 - 4 * xpos
    yn = me + 4 - 8 * ypos
    dg = yn + 2 - 4 * xpos
    sx = xn + 1 - 2 * core
    sy = yn + 1 - 2 * core
    sd = dg + 1 - 2 * core

    def rows(dev):
        return pl.ds(pl.multiple_of(dev * ROWS, 16), ROWS)

    LO, HI, ALL = pl.ds(0, NP // 2), pl.ds(NP // 2, NP // 2), pl.ds(0, NP)
    kinds = ((LO, me, xn, xn), (HI, me, xn, xn), (HI, me, yn, yn), (LO, me, yn, yn), (ALL, me, sib, sib),
             (LO, xn, yn, dg), (HI, yn, xn, dg), (ALL, xn, sib, sx), (ALL, yn, sib, sy), (ALL, dg, sib, sd))

    def send(c, kind):
        ps, origin, target, _ = kinds[kind]
        part = vbuf.at[c, ps, rows(origin), :]
        return pltpu.make_async_remote_copy(part, part, send_sem.at[c, kind], recv_sem.at[c, kind],
                                            device_id=(target,), device_id_type=MESH)

    def landed(c, kind):
        ps, _, target, origin = kinds[kind]
        part = vbuf.at[c, ps, rows(origin), :]
        pltpu.make_async_remote_copy(part, part, send_sem.at[c, kind], recv_sem.at[c, kind],
                                     device_id=(target,), device_id_type=MESH).wait_recv()

    def send_own(c):
        for kind in (0, 2, 1, 3, 4):
            send(c, kind).start()

    def relay_half(c):
        landed(c, 0)
        send(c, 5).start()
        landed(c, 2)
        send(c, 6).start()

    def relay_sib(c):
        landed(c, 1)
        send(c, 7).start()
        landed(c, 3)
        send(c, 8).start()

    def relay_diag(c):
        landed(c, 5)
        landed(c, 6)
        send(c, 9).start()

    def arrived(c):
        for kind in (4, 7, 8, 9):
            landed(c, kind)

    def local_chunk(c):
        return pltpu.make_async_copy(v0_h.at[c], vbuf.at[c], v0_sem.at[c])

    barrier = pltpu.get_barrier_semaphore()
    for off in range(1, NDEV):
        pl.semaphore_signal(barrier, inc=1, device_id=(lax.rem(me + off, NDEV),), device_id_type=MESH)
    pl.semaphore_wait(barrier, NDEV - 1)

    local_chunk(0).start()
    loads = [pltpu.make_async_copy(left_h, left, load_sem.at[0]),
             pltpu.make_async_copy(kron_h, kron, load_sem.at[1]),
             pltpu.make_async_copy(slab_h, vecs.at[0], load_sem.at[2])]
    for cp in loads:
        cp.start()
    for c in range(1, NCH):
        local_chunk(c).start()
    vecs[1] = jnp.zeros((SLAB, BOND), jnp.float32)
    for cp in loads:
        cp.wait()

    def fetch(u):
        kg, c, slot = lax.rem(u, NKG), lax.div(u, NKG), lax.rem(u, 2)
        return [pltpu.make_async_copy(
            right_h.at[kg * KG + k, :, pl.ds(pl.multiple_of(c * LANES, LANES), LANES)],
            rblk.at[slot, :, pl.ds(k * LANES, LANES)], r_sem.at[slot, k]) for k in range(KG)]

    def stage_left(u):
        kg, c = lax.rem(u, NKG), lax.div(u, NKG)
        lhs = left[pl.ds(pl.multiple_of(kg * KG * ROWS, 64), KG * ROWS), :]
        for g in range(NP // 4):
            rhs = jnp.concatenate([vbuf[c, 4 * g + i] for i in range(4)], axis=1)
            o = jnp.dot(lhs, rhs, preferred_element_type=jnp.float32).astype(jnp.bfloat16)
            for i in range(4):
                ubuf[4 * g + i] = o[:, i * LANES:(i + 1) * LANES]

    def stage_pair(u):
        kg = lax.rem(u, NKG)
        for k in range(KG):
            rhs = jnp.concatenate([ubuf[:, k * ROWS + g * 16:k * ROWS + (g + 1) * 16, :].reshape(256, LANES)
                                   for g in range(ROWS // 16)], axis=1)
            o = jnp.dot(kron[kg * KG + k], rhs, preferred_element_type=jnp.float32).astype(jnp.bfloat16)
            for g in range(ROWS // 16):
                for q in range(NP):
                    zbuf[q * ROWS + g * 16:q * ROWS + (g + 1) * 16, k * LANES:(k + 1) * LANES] = (
                        o[q * 16:(q + 1) * 16, g * LANES:(g + 1) * LANES])

    def stage_right(u):
        slot = lax.rem(u, 2)
        for n0, n1 in NS:
            o = lax.dot_general(rblk[slot], zbuf[n0:n1, :], (((1,), (1,)), ((), ())),
                                preferred_element_type=jnp.float32)
            sig[:, n0:n1] += o

    def fold(x):
        return jnp.sum(x.reshape(-1, 8, LANES), axis=0)

    def one_step(j, beta_prev):
        cur, prv = lax.rem(j, 2), lax.rem(j + 1, 2)

        def gather_at(u):
            c, r = lax.div(u, NKG), lax.rem(u, NKG)

            @pl.when((j == 0) & (r == 0))
            def _():
                local_chunk(c).wait()

            @pl.when((j > 0) & (r == 0))
            def _():
                arrived(c)

            @pl.when((j > 0) & (r == 1) & (c < NCH - 1))
            def _():
                relay_half(c + 1)

            @pl.when((j > 0) & (r == 1) & (c < NCH - 2))
            def _():
                send_own(c + 2)

            @pl.when((j > 0) & (r == 2) & (c < NCH - 1))
            def _():
                relay_sib(c + 1)

            @pl.when((j > 0) & (r == 3) & (c < NCH - 1))
            def _():
                relay_diag(c + 1)

        for cp in fetch(0):
            cp.start()
        sig[...] = jnp.zeros((BOND, SLAB), jnp.float32)

        @pl.when(j > 0)
        def _():
            relay_half(0)
            send_own(1)
            relay_sib(0)
            relay_diag(0)

        gather_at(0)
        stage_left(0)
        gather_at(1)
        for cp in fetch(1):
            cp.start()
        stage_pair(0)
        stage_left(1)

        def unit(u, carry):
            gather_at(u)
            for cp in fetch(u - 2):
                cp.wait()
            stage_right(u - 2)
            stage_pair(u - 1)
            stage_left(u)
            for cp in fetch(u):
                cp.start()
            return carry

        lax.fori_loop(2, UNITS, unit, 0)
        for cp in fetch(UNITS - 2):
            cp.wait()
        stage_right(UNITS - 2)
        stage_pair(UNITS - 1)
        for cp in fetch(UNITS - 1):
            cp.wait()
        stage_right(UNITS - 1)

        def first(i, sums):
            a_sum, b_sum, v_sum = sums
            at = pl.ds(pl.multiple_of(i * LANES, LANES), LANES)
            for c in range(NCH):
                cs = slice(c * LANES, (c + 1) * LANES)
                tile = sig[cs, at].T
                v = vecs[cur, at, cs]
                s = tile - beta_prev * vecs[prv, at, cs]
                vecs[prv, at, cs] = s
                a_sum = a_sum + fold(tile * v)
                b_sum = b_sum + fold(s * v)
                v_sum = v_sum + fold(v * v)
            return a_sum, b_sum, v_sum

        zero = jnp.zeros((8, LANES), jnp.float32)
        a_sum, b_sum, v_sum = lax.fori_loop(0, SLAB // LANES, first, (zero, zero, zero), unroll=2)
        a_loc, b_loc, v_loc = jnp.sum(a_sum), jnp.sum(b_sum), jnp.sum(v_sum)
        a_row = jnp.full((8, LANES), a_loc)
        v_row = jnp.full((8, LANES), v_loc)
        fit = jnp.where(v_row > 0, jnp.full((8, LANES), b_loc) / jnp.where(v_row > 0, v_row, 1.0), 0.0)
        fit_row = fit[0:1, :]

        def second(i, n_sum):
            at = pl.ds(pl.multiple_of(i * LANES, LANES), LANES)
            for c in range(NCH):
                cs = slice(c * LANES, (c + 1) * LANES)
                d = vecs[prv, at, cs] - fit_row * vecs[cur, at, cs]
                n_sum = n_sum + fold(d * d)
            return n_sum

        n_loc = jnp.sum(lax.fori_loop(0, SLAB // LANES, second, zero, unroll=2))

        @pl.when(j > 0)
        def _():
            def sent(c, carry):
                for kind in range(len(kinds)):
                    send(c, kind).wait_send()
                return carry
            lax.fori_loop(0, NCH, sent, 0)

        @pl.when(j > 0)
        def _():
            pltpu.make_async_copy(vecs.at[cur], vout_h.at[j - 1], out_sem.at[0]).wait()

        row_id = lax.broadcasted_iota(jnp.int32, (8, LANES), 0)
        mine[...] = jnp.where(row_id == 0, a_row, jnp.where(
            row_id == 1, v_row, jnp.where(row_id == 2, fit, jnp.full((8, LANES), n_loc))))
        par = lax.rem(j, 2)
        exch[par, me] = mine[...]
        copies = []
        for off in range(1, NDEV):
            copies.append(pltpu.make_async_remote_copy(
                mine, exch.at[par, me], xs_sem.at[off - 1], xr_sem.at[par, off - 1],
                device_id=(lax.rem(me + off, NDEV),), device_id_type=MESH))
        for cp in copies:
            cp.start()
        for off in range(1, NDEV):
            src = lax.rem(me + NDEV - off, NDEV)
            pltpu.make_async_remote_copy(
                mine, exch.at[par, src], xs_sem.at[off - 1], xr_sem.at[par, off - 1],
                device_id=(src,), device_id_type=MESH).wait_recv()
        for cp in copies:
            cp.wait_send()
        total = exch[par, 0]
        for d in range(1, NDEV):
            total = total + exch[par, d]
        alpha = total[0:1, :] * (1.0 / ELEMS)
        square = jnp.zeros((1, LANES), jnp.float32)
        for d in range(NDEV):
            part = exch[par, d]
            gap = alpha - part[2:3, :]
            square = square + (part[3:4, :] + gap * gap * part[1:2, :])
        beta = jnp.sqrt(square * (1.0 / ELEMS))
        inv = 1.0 / beta
        ab_ref[j] = jnp.concatenate([alpha, beta] + [alpha] * 6, axis=0)

        for c in range(NCH):
            cs = slice(c * LANES, (c + 1) * LANES)

            def third(p, carry, c=c, cs=cs):
                at = pl.ds(pl.multiple_of(p * ROWS, 16), ROWS)
                n = (vecs[prv, at, cs] - alpha * vecs[cur, at, cs]) * inv
                vecs[prv, at, cs] = n
                vbuf[c, p, rows(me), :] = n.astype(jnp.bfloat16)
                return carry

            lax.fori_loop(0, NP, third, 0, unroll=4)
            if c == 1:
                @pl.when(j < STEPS - 1)
                def _():
                    send_own(0)
        pltpu.make_async_copy(vecs.at[prv], vout_h.at[j], out_sem.at[0]).start()
        return beta

    lax.fori_loop(0, STEPS, one_step, jnp.zeros((1, LANES), jnp.float32))
    pltpu.make_async_copy(vecs.at[STEPS % 2], vout_h.at[STEPS - 1], out_sem.at[0]).wait()


def lanczos(v0_low, v0_slab, left, kron, right):
    dma = pltpu.SemaphoreType.DMA
    return pl.pallas_call(
        kernel,
        out_shape=(jax.ShapeDtypeStruct((STEPS, SLAB, BOND), jnp.float32),
                   jax.ShapeDtypeStruct((STEPS, 8, LANES), jnp.float32)),
        in_specs=[pl.BlockSpec(memory_space=pl.ANY)] * 5,
        out_specs=(pl.BlockSpec(memory_space=pl.ANY), pl.BlockSpec(memory_space=pltpu.VMEM)),
        scratch_shapes=[
            pltpu.VMEM((NCH, NP, BOND, LANES), jnp.bfloat16),
            pltpu.VMEM((TERMS * ROWS, BOND), jnp.bfloat16),
            pltpu.VMEM((TERMS, 256, 256), jnp.bfloat16),
            pltpu.VMEM((2, BOND, KG * LANES), jnp.bfloat16),
            pltpu.VMEM((BOND, SLAB), jnp.float32),
            pltpu.VMEM((NP, KG * ROWS, LANES), jnp.bfloat16),
            pltpu.VMEM((SLAB, KG * LANES), jnp.bfloat16),
            pltpu.VMEM((2, SLAB, BOND), jnp.float32),
            pltpu.VMEM((8, LANES), jnp.float32),
            pltpu.VMEM((2, NDEV, 8, LANES), jnp.float32),
            dma((3,)), dma((NCH,)), dma((2, KG)), dma((1,)),
            dma((NCH, 10)), dma((NCH, 10)), dma((NDEV - 1,)), dma((2, NDEV - 1)),
        ],
        compiler_params=pltpu.CompilerParams(collective_id=0, has_side_effects=True, vmem_limit_bytes=67043328),
    )(v0_low, v0_slab, left, kron, right)


def solution(mesh):
    def local_run(psi_init, left_env, op_pair, right_env):
        row_start = lax.axis_index('terms') * ROWS
        right = lax.all_gather(right_env, 'terms', axis=0, tiled=True)
        left = lax.all_to_all(left_env, 'terms', split_axis=1, concat_axis=0, tiled=True).reshape(TERMS * ROWS, BOND)
        pair = lax.all_gather(op_pair, 'terms', axis=0, tiled=True)
        eye = jnp.eye(16, dtype=jnp.bfloat16)
        kron = (pair[:, :, None, :, None] * eye[None, None, :, None, :]).reshape(TERMS, 256, 256)
        psi = psi_init.reshape(BOND, NP, BOND)
        norm = jnp.sqrt(jnp.sum(psi * psi) / ELEMS)
        v0 = psi / norm
        v0_low = v0.astype(jnp.bfloat16).reshape(BOND, NP, NCH, LANES).transpose(2, 1, 0, 3)
        v0_own = lax.dynamic_slice_in_dim(psi, row_start, ROWS, 0) / norm
        v0_slab = v0_own.transpose(1, 0, 2).reshape(SLAB, BOND)
        vout, ab = lanczos(v0_low, v0_slab, left, kron, right)
        later = vout.reshape(STEPS, NP, ROWS, BOND).transpose(0, 2, 1, 3)
        vectors = jnp.concatenate([v0_own[None], later], axis=0).reshape(STEPS + 1, ROWS, 4, 4, BOND)
        return vectors, ab[:, 0, 0], ab[:, 1, 0]

    return jax.shard_map(local_run, mesh=mesh, in_specs=(P(), P('terms'), P('terms'), P('terms')),
                         out_specs=(P(None, 'terms'), P(), P()), check_vma=False)
```

```python
import jax
import jax.numpy as jnp
from jax import lax
from jax.experimental import pallas as pl
from jax.experimental.pallas import tpu as pltpu
from jax.sharding import PartitionSpec as P

STEPS = 6
BOND = 896
NP = 16
TERMS = 16
NDEV = 8
ROWS = BOND // NDEV
LANES = 128
NCH = BOND // LANES
KG = 4
NKG = TERMS // KG
UNITS = NCH * NKG
SLAB = NP * ROWS
SLOTS = SLAB // LANES
ELEMS = BOND * NP * BOND
MESH = pl.DeviceIdType.MESH
NS = ((0, 4), (4, 8), (8, 12), (12, 14))


def kernel(psi_h, left_h, pair_h, right_h, kry_h, rall_h, ab_ref,
           vbuf, left, wall, kron, rblk, sig, ubuf, zbuf, vec, scale, mine, exch,
           slab_sem, psi_sem, own_sem, ls_sem, lr_sem, ws_sem, wr_sem,
           r_sem, out_sem, send_sem, recv_sem, xs_sem, xr_sem):
    me = lax.axis_index('terms')
    core = lax.rem(me, 2)
    xpos = lax.rem(lax.div(me, 2), 2)
    ypos = lax.div(me, 4)
    sib = me + 1 - 2 * core
    xn = me + 2 - 4 * xpos
    yn = me + 4 - 8 * ypos
    dg = yn + 2 - 4 * xpos
    sx = xn + 1 - 2 * core
    sy = yn + 1 - 2 * core
    sd = dg + 1 - 2 * core
    others = (sib, xn, sx, yn, sy, dg, sd)

    def rows(dev):
        return pl.ds(pl.multiple_of(dev * ROWS, 16), ROWS)

    def lanes(c):
        return pl.ds(pl.multiple_of(c * LANES, LANES), LANES)

    def remote(src, dst, ssem, rsem, target):
        return pltpu.make_async_remote_copy(src, dst, ssem, rsem, device_id=(target,), device_id_type=MESH)

    v_kinds = ((0, 4, me, xn, xn), (0, 4, me, yn, yn), (0, 4, me, sib, sib), (0, 2, xn, yn, dg), (2, 2, yn, xn, dg),
               (0, 4, xn, sib, sx), (0, 4, yn, sib, sy), (0, 4, dg, sib, sd))
    NV = len(v_kinds)

    def v_part(first, count, origin, q):
        return vbuf.at[lax.div(q, 4), pl.ds(4 * lax.rem(q, 4) + first, count), rows(origin), :]

    def v_send(q, kind):
        first, count, origin, target, _ = v_kinds[kind]
        part = v_part(first, count, origin, q)
        remote(part, part, send_sem.at[kind], recv_sem.at[q * NV + kind], target).start()

    def v_landed(q, kind):
        first, count, _, target, origin = v_kinds[kind]
        part = v_part(first, count, origin, q)
        remote(part, part, send_sem.at[kind], recv_sem.at[q * NV + kind], target).wait_recv()

    def v_sent(kind):
        first, count, origin, target, _ = v_kinds[kind]
        part = vbuf.at[:, pl.ds(0, 4 * count), rows(origin), :]
        remote(part, part, send_sem.at[kind], recv_sem.at[kind], target).wait_send()

    def send_own(q):
        for kind in (0, 1, 2):
            v_send(q, kind)

    def relay_xy(q):
        v_landed(q, 0)
        v_send(q, 3)
        v_send(q, 5)
        v_landed(q, 1)
        v_send(q, 4)
        v_send(q, 6)

    def relay_diag(q):
        v_landed(q, 3)
        v_landed(q, 4)
        v_send(q, 7)

    def arrived(q):
        for kind in (2, 5, 6, 7):
            v_landed(q, kind)

    LO, HI, ALL = (0, 1), (1, 1), (0, 2)
    r_kinds = ((LO, me, xn, xn), (HI, me, xn, xn), (HI, me, yn, yn), (LO, me, yn, yn), (ALL, me, sib, sib),
               (LO, xn, yn, dg), (HI, yn, xn, dg), (ALL, xn, sib, sx), (ALL, yn, sib, sy), (ALL, dg, sib, sd))
    NR = len(r_kinds)

    def r_part(half, origin, c):
        return rall_h.at[pl.ds(2 * origin + half[0], half[1]), :, lanes(c)]

    def r_send(c, kind):
        half, origin, target, _ = r_kinds[kind]
        dst = r_part(half, origin, c)
        src = right_h.at[pl.ds(half[0], half[1]), :, lanes(c)] if kind < 5 else dst
        remote(src, dst, send_sem.at[kind], recv_sem.at[c * NR + kind], target).start()

    def r_landed(c, kind):
        half, _, target, origin = r_kinds[kind]
        part = r_part(half, origin, c)
        remote(part, part, send_sem.at[kind], recv_sem.at[c * NR + kind], target).wait_recv()

    def r_sent(kind):
        half, origin, target, _ = r_kinds[kind]
        part = rall_h.at[pl.ds(2 * origin + half[0], half[1])]
        remote(part, part, send_sem.at[kind], recv_sem.at[kind], target).wait_send()

    def left_copy(n):
        return remote(left_h.at[:, rows(others[n]), :], left.at[pl.ds(2 * me, 2)], ls_sem.at[n], lr_sem.at[n], others[n])

    def left_landed(n):
        part = left.at[pl.ds(2 * others[n], 2)]
        remote(part, part, ls_sem.at[n], lr_sem.at[n], others[n]).wait_recv()

    def pair_copy(n):
        return remote(pair_h, wall.at[pl.ds(2 * me, 2)], ws_sem.at[n], wr_sem.at[n], others[n])

    def pair_landed(n):
        part = wall.at[pl.ds(2 * others[n], 2)]
        remote(part, part, ws_sem.at[n], wr_sem.at[n], others[n]).wait_recv()

    def psi_copy(n):
        c, p, slot = lax.div(n, NP), lax.rem(n, NP), lax.rem(n, SLOTS)
        return pltpu.make_async_copy(psi_h.at[:, lax.div(p, 4), lax.rem(p, 4), lanes(c)], sig.at[:, lanes(slot)],
                                     psi_sem.at[slot])

    def vector_out(j):
        return [pltpu.make_async_copy(vec.at[pl.ds(p * ROWS, ROWS), :], kry_h.at[j, :, p // 4, p % 4, :],
                                      out_sem.at[p]) for p in range(NP)]

    def fold(x):
        return jnp.sum(x.reshape(-1, 8, LANES), axis=0)

    def exchange_start(par):
        exch[par, me] = mine[...]
        copies = [remote(mine, exch.at[par, me], xs_sem.at[n], xr_sem.at[par, n], others[n]) for n in range(NDEV - 1)]
        for cp in copies:
            cp.start()
        return copies

    def exchange_wait(par, copies):
        for n in range(NDEV - 1):
            remote(mine, exch.at[par, others[n]], xs_sem.at[n], xr_sem.at[par, n], others[n]).wait_recv()
        for cp in copies:
            cp.wait_send()

    barrier = pltpu.get_barrier_semaphore()
    for n in range(NDEV - 1):
        pl.semaphore_signal(barrier, inc=1, device_id=(others[n],), device_id_type=MESH)
    slab = [pltpu.make_async_copy(psi_h.at[rows(me), p // 4, p % 4, :], vec.at[pl.ds(p * ROWS, ROWS), :],
                                  slab_sem.at[p]) for p in range(NP)]
    for cp in slab:
        cp.start()
    own = [pltpu.make_async_copy(pair_h, wall.at[pl.ds(2 * me, 2)], own_sem.at[0]),
           pltpu.make_async_copy(left_h.at[:, rows(me), :], left.at[pl.ds(2 * me, 2)], own_sem.at[1])]
    for cp in own:
        cp.start()
    for n in range(SLOTS):
        psi_copy(n).start()
    zero = jnp.zeros((8, LANES), jnp.float32)
    for cp in slab:
        cp.wait()

    def squares(i, acc):
        at = pl.ds(pl.multiple_of(i * LANES, LANES), LANES)
        for c in range(NCH):
            x = vec[at, c * LANES:(c + 1) * LANES]
            acc = acc + fold(x * x)
        return acc

    mine[...] = jnp.full((8, LANES), jnp.sum(lax.fori_loop(0, SLOTS, squares, zero, unroll=2)))
    with jax.named_scope('barrier'):
        pl.semaphore_wait(barrier, NDEV - 1)
    copies = exchange_start(1)
    for n in range(NDEV - 1):
        pair_copy(n).start()
    for n in range(NDEV - 1):
        left_copy(n).start()

    def r_own(c):
        for kind in (4, 0, 2, 1, 3):
            r_send(c, kind)

    r_own(0)
    with jax.named_scope('exch0'):
        exchange_wait(1, copies)
    total = exch[1, 0]
    for d in range(1, NDEV):
        total = total + exch[1, d]
    scale[...] = 1.0 / jnp.sqrt(total * (1.0 / ELEMS))

    def normalise(i, carry):
        at = pl.ds(pl.multiple_of(i * LANES, LANES), LANES)
        for c in range(NCH):
            cs = slice(c * LANES, (c + 1) * LANES)
            vec[at, cs] = vec[at, cs] * scale[0:1, :]
        return carry

    lax.fori_loop(0, SLOTS, normalise, 0, unroll=2)
    for cp in vector_out(0):
        cp.start()

    def piece(n, carry):
        psi_copy(n).wait()
        vbuf[lax.div(n, NP), lax.rem(n, NP)] = (sig[:, lanes(lax.rem(n, SLOTS))] * scale[0:1, :]).astype(jnp.bfloat16)

        @pl.when(n + SLOTS < NP * NCH)
        def _():
            psi_copy(n + SLOTS).start()
        return carry

    with jax.named_scope('convert'):
        lax.fori_loop(0, NP * NCH, piece, 0)

    for n in range(NDEV - 1):
        pair_landed(n)
    for cp in own:
        cp.wait()
    spread = (lax.div(lax.broadcasted_iota(jnp.int32, (256, 16), 0), 16)
              == lax.broadcasted_iota(jnp.int32, (256, 16), 1)).astype(jnp.float32).astype(jnp.bfloat16)
    same = (lax.rem(lax.broadcasted_iota(jnp.int32, (256, 256), 0), 16)
            == lax.rem(lax.broadcasted_iota(jnp.int32, (256, 256), 1), 16))

    def expand(k, carry):
        tall = jnp.dot(spread, wall[k], preferred_element_type=jnp.float32).astype(jnp.bfloat16)
        full = lax.dot_general(tall, spread, (((1,), (1,)), ((), ())), preferred_element_type=jnp.float32)
        kron[k] = jnp.where(same, full, 0.0).astype(jnp.bfloat16)
        return carry

    with jax.named_scope('kron'):
        lax.fori_loop(0, TERMS, expand, 0, unroll=4)
    sig[...] = jnp.zeros((BOND, SLAB), jnp.float32)
    with jax.named_scope('leftwait'):
        for n in range(NDEV - 1):
            left_landed(n)

    chip = lax.div(me, 2)

    def group(rel):
        return chip + lax.rem(rel, 2) * (1 - 2 * xpos) + lax.div(rel, 2) * (2 - 4 * ypos)

    def fetch_start(w):
        c, rel, slot = lax.div(w, NKG), lax.rem(w, NKG), lax.rem(w, 2)
        kg = group(rel)
        for k in range(KG):
            dst = rblk.at[slot, :, pl.ds(k * LANES, LANES)]
            here = (rel == 0) & (core == k // 2)

            @pl.when(here)
            def _():
                pltpu.make_async_copy(right_h.at[k % 2, :, lanes(c)], dst, r_sem.at[slot, k]).start()

            @pl.when(jnp.logical_not(here))
            def _():
                pltpu.make_async_copy(rall_h.at[kg * KG + k, :, lanes(c)], dst, r_sem.at[slot, k]).start()

    def fetch_wait(slot):
        for k in range(KG):
            pltpu.make_async_copy(rall_h.at[k, :, lanes(0)], rblk.at[slot, :, pl.ds(k * LANES, LANES)],
                                  r_sem.at[slot, k]).wait()

    def stage_left(c, g):
        rhs = jnp.concatenate([vbuf[c, 4 * g + i] for i in range(4)], axis=1)
        for kg in range(NKG):
            lhs = left[kg * KG:(kg + 1) * KG].reshape(KG * ROWS, BOND)
            o = jnp.dot(lhs, rhs, preferred_element_type=jnp.float32).astype(jnp.bfloat16)
            for i in range(4):
                ubuf[4 * g + i, kg * KG * ROWS:(kg + 1) * KG * ROWS, :] = o[:, i * LANES:(i + 1) * LANES]

    def stage_pair(k):
        rhs = jnp.concatenate([ubuf[:, k * ROWS + g * 16:k * ROWS + (g + 1) * 16, :].reshape(256, LANES)
                               for g in range(ROWS // 16)], axis=1)
        o = jnp.dot(kron[k], rhs, preferred_element_type=jnp.float32).astype(jnp.bfloat16)
        kg, at = k // KG, (k % KG) * LANES
        for g in range(ROWS // 16):
            for q in range(NP):
                zbuf[kg, q * ROWS + g * 16:q * ROWS + (g + 1) * 16, at:at + LANES] = (
                    o[q * 16:(q + 1) * 16, g * LANES:(g + 1) * LANES])

    def stage_right(rel, slot, part):
        n0, n1 = NS[part][0] * LANES, NS[part][1] * LANES
        o = lax.dot_general(rblk[slot], zbuf[group(rel), n0:n1, :], (((1,), (1,)), ((), ())),
                            preferred_element_type=jnp.float32)
        sig[:, n0:n1] += o

    def one_step(j, carry):
        beta_prev, cross = carry

        def r_before(q):
            c, g = lax.div(q, NKG), lax.rem(q, NKG)

            @pl.when((g == 3) & (c < NCH))
            def _():
                for kind in (0, 2, 1, 3):
                    r_landed(c, kind)
                for kind in (5, 6, 7, 8):
                    r_send(c, kind)

            @pl.when((g == 3) & (c < NCH - 1))
            def _():
                r_own(c + 1)

            @pl.when((g == 1) & (c > 0))
            def _():
                r_landed(c - 1, 5)
                r_landed(c - 1, 6)
                r_send(c - 1, 9)

        def before(q):
            @pl.when(j == 0)
            def _():
                r_before(q)

            @pl.when(j > 0)
            def _():
                @pl.when(q < UNITS - 1)
                def _():
                    relay_diag(q + 1)

                @pl.when(q < UNITS - 2)
                def _():
                    relay_xy(q + 2)

                @pl.when(q < UNITS - 4)
                def _():
                    send_own(q + 4)

                arrived(q)

        def first_chunk(g):
            @pl.when(j > 0)
            def _():
                relay_xy(g + 1)
                send_own(g + 3)
                relay_diag(g)
                arrived(g)

        def after(q):
            @pl.when(j == 0)
            def _():
                c, g = lax.div(q, NKG), lax.rem(q, NKG)
                for at, lag, kind in ((2, 0, 4), (3, 0, 7), (0, 1, 8), (1, 1, 9)):
                    @pl.when(g == at)
                    def _(lag=lag, kind=kind):
                        r_landed(c - lag, kind)

            fetch_start(q - 2)

        @pl.when(j > 0)
        def _():
            relay_xy(0)
            send_own(2)

        def opening(g, carry):
            with jax.named_scope('first'):
                first_chunk(g)
            with jax.named_scope('L'):
                stage_left(0, g)
            return carry

        lax.fori_loop(0, 2, opening, 0)
        first_chunk(2)
        with jax.named_scope('L'):
            stage_left(0, 2)
        with jax.named_scope('r1'):
            after(2)

            @pl.when(j == 0)
            def _():
                r_before(3)
            first_chunk(3)
        with jax.named_scope('LW'):
            stage_left(0, 3)
            for k in range(TERMS):
                stage_pair(k)
        with jax.named_scope('r2'):
            after(3)

            @pl.when(j > 0)
            def _():
                relay_diag(4)
                relay_xy(5)
                send_own(7)

        def chunk(c, carry):
            def unit(g, carry):
                q, slot = NKG * c + g, lax.rem(g, 2)
                with jax.named_scope('before'):
                    before(q)
                with jax.named_scope('RL'):
                    fetch_wait(slot)
                    for part in range(len(NS)):
                        stage_right(g, slot, part)
                    stage_left(c, g)
                with jax.named_scope('after'):
                    after(q)
                return carry

            lax.fori_loop(0, NKG - 1, unit, 0)
            q = NKG * c + NKG - 1
            with jax.named_scope('before'):
                before(q)
            with jax.named_scope('LRW'):
                fetch_wait(1)
                stage_left(c, NKG - 1)
                for part in range(len(NS)):
                    stage_right(NKG - 1, 1, part)
                for k in range(TERMS):
                    stage_pair(k)
            with jax.named_scope('after'):
                after(q)
            return carry

        lax.fori_loop(1, NCH, chunk, 0)

        def tail(g, carry):
            @pl.when(j == 0)
            def _():
                r_before(UNITS + g)
            with jax.named_scope('tail'):
                fetch_wait(lax.rem(g, 2))
                for part in range(len(NS)):
                    stage_right(g, lax.rem(g, 2), part)

            @pl.when(g < 2)
            def _():
                after(UNITS + g)
            return carry

        lax.fori_loop(0, NKG - 1, tail, 0)

        with jax.named_scope('sent'):
            @pl.when(j == 0)
            def _():
                for kind in range(NR):
                    r_sent(kind)
                for n in range(NDEV - 1):
                    left_copy(n).wait_send()
                    pair_copy(n).wait_send()

            @pl.when(j > 0)
            def _():
                for kind in range(NV):
                    v_sent(kind)

        with jax.named_scope('last'):
            fetch_wait(1)
            b_sum, v_sum = zero, zero
            for part in range(len(NS)):
                stage_right(NKG - 1, 1, part)
                for i in range(*NS[part]):
                    at = slice(i * LANES, (i + 1) * LANES)
                    for c in range(NCH):
                        cs = slice(c * LANES, (c + 1) * LANES)
                        s = sig[cs, at].T
                        v = vec[at, cs]
                        sig[cs, at] = s
                        b_sum = b_sum + fold(s * v)
                        v_sum = v_sum + fold(v * v)

        b_row = jnp.full((8, LANES), jnp.sum(b_sum))
        v_row = jnp.full((8, LANES), jnp.sum(v_sum))
        a_row = b_row + beta_prev * cross
        fit = jnp.where(v_row > 0, b_row / jnp.where(v_row > 0, v_row, 1.0), 0.0)
        fit_row = fit[0:1, :]

        def second(i, n_sum):
            at = pl.ds(pl.multiple_of(i * LANES, LANES), LANES)
            for c in range(NCH):
                cs = slice(c * LANES, (c + 1) * LANES)
                d = sig[cs, at] - fit_row * vec[at, cs]
                n_sum = n_sum + fold(d * d)
            return n_sum

        with jax.named_scope('pass2'):
            n_loc = jnp.sum(lax.fori_loop(0, SLOTS, second, zero, unroll=2))
        for cp in vector_out(j):
            cp.wait()

        row_id = lax.broadcasted_iota(jnp.int32, (8, LANES), 0)
        mine[...] = jnp.where(row_id == 0, a_row, jnp.where(
            row_id == 1, v_row, jnp.where(row_id == 2, fit, jnp.full((8, LANES), n_loc))))
        par = lax.rem(j, 2)
        with jax.named_scope('exch'):
            exchange_wait(par, exchange_start(par))
        total = exch[par, 0]
        for d in range(1, NDEV):
            total = total + exch[par, d]
        alpha = total[0:1, :] * (1.0 / ELEMS)
        square = jnp.zeros((1, LANES), jnp.float32)
        for d in range(NDEV):
            part = exch[par, d]
            gap = alpha - part[2:3, :]
            square = square + (part[3:4, :] + gap * gap * part[1:2, :])
        beta = jnp.sqrt(square * (1.0 / ELEMS))
        inv = 1.0 / beta
        ab_ref[j] = jnp.concatenate([alpha, beta] + [alpha] * 6, axis=0)

        def third(c, x_sum):
            cs = lanes(c)
            for i in range(SLOTS):
                at = slice(i * LANES, (i + 1) * LANES)
                v = vec[at, cs]
                n = (sig[cs, at] - alpha * v) * inv
                x_sum = x_sum + fold(v * n)
                vec[at, cs] = n
                low = n.astype(jnp.bfloat16)
                for t in range(8):
                    p, a = divmod(8 * i + t, ROWS // 16)
                    vbuf[c, p, pl.ds(pl.multiple_of(me * ROWS + 16 * a, 16), 16), :] = low[16 * t:16 * t + 16]
                sig[cs, at] = (v * -beta).T

            @pl.when((c == 1) & (j < STEPS - 1))
            def _():
                send_own(0)
                send_own(1)
            return x_sum

        with jax.named_scope('pass3'):
            x_sum = lax.fori_loop(0, NCH, third, zero)
        for cp in vector_out(j + 1):
            cp.start()
        return beta, jnp.full((8, LANES), jnp.sum(x_sum))

    lax.fori_loop(0, STEPS, one_step, (jnp.zeros((1, LANES), jnp.float32), zero))
    for cp in vector_out(STEPS):
        cp.wait()


def lanczos(psi, left, pair, right):
    dma = pltpu.SemaphoreType.DMA
    return pl.pallas_call(
        kernel,
        out_shape=(jax.ShapeDtypeStruct((STEPS + 1, ROWS, 4, 4, BOND), jnp.float32),
                   jax.ShapeDtypeStruct((TERMS, BOND, BOND), jnp.bfloat16),
                   jax.ShapeDtypeStruct((STEPS, 8, LANES), jnp.float32)),
        in_specs=[pl.BlockSpec(memory_space=pl.ANY)] * 4,
        out_specs=(pl.BlockSpec(memory_space=pl.ANY), pl.BlockSpec(memory_space=pl.ANY),
                   pl.BlockSpec(memory_space=pltpu.VMEM)),
        scratch_shapes=[
            pltpu.VMEM((NCH, NP, BOND, LANES), jnp.bfloat16),
            pltpu.VMEM((TERMS, ROWS, BOND), jnp.bfloat16),
            pltpu.VMEM((TERMS, 16, 16), jnp.bfloat16),
            pltpu.VMEM((TERMS, 256, 256), jnp.bfloat16),
            pltpu.VMEM((2, BOND, KG * LANES), jnp.bfloat16),
            pltpu.VMEM((BOND, SLAB), jnp.float32),
            pltpu.VMEM((NP, TERMS * ROWS, LANES), jnp.bfloat16),
            pltpu.VMEM((NKG, SLAB, KG * LANES), jnp.bfloat16),
            pltpu.VMEM((SLAB, BOND), jnp.float32),
            pltpu.VMEM((8, LANES), jnp.float32),
            pltpu.VMEM((8, LANES), jnp.float32),
            pltpu.VMEM((2, NDEV, 8, LANES), jnp.float32),
            dma((NP,)), dma((SLOTS,)), dma((2,)), dma((NDEV - 1,)), dma((NDEV - 1,)), dma((NDEV - 1,)), dma((NDEV - 1,)),
            dma((2, KG)), dma((NP,)), dma((10,)), dma((UNITS * 8,)), dma((NDEV - 1,)), dma((2, NDEV - 1)),
        ],
        compiler_params=pltpu.CompilerParams(collective_id=0, has_side_effects=True, vmem_limit_bytes=67043328),
    )(psi, left, pair, right)


def solution(mesh):
    def local_run(psi_init, left_env, op_pair, right_env):
        vectors, _, ab = lanczos(psi_init, left_env, op_pair, right_env)
        return vectors, ab[:, 0, 0], ab[:, 1, 0]

    return jax.shard_map(local_run, mesh=mesh, in_specs=(P(), P('terms'), P('terms'), P('terms')),
                         out_specs=(P(None, 'terms'), P(), P()), check_vma=False)
```

```python
import jax
import jax.numpy as jnp
from jax import lax
from jax.experimental import pallas as pl
from jax.experimental.pallas import tpu as pltpu
from jax.sharding import PartitionSpec as P

STEPS = 6
BOND = 896
NP = 16
TERMS = 16
NDEV = 8
ROWS = BOND // NDEV
LANES = 128
NCH = BOND // LANES
KG = 4
NKG = TERMS // KG
UNITS = NCH * NKG
SLAB = NP * ROWS
SLOTS = SLAB // LANES
ELEMS = BOND * NP * BOND
MESH = pl.DeviceIdType.MESH
NS = ((0, 4), (4, 8), (8, 12), (12, 14))


def kernel(psi_h, left_h, pair_h, right_h, kry_h, rall_h, ab_ref,
           vbuf, left, wall, kron, rblk, sig, ubuf, zbuf, vec, scale, mine, exch,
           slab_sem, psi_sem, own_sem, rest_sem, ls_sem, lr_sem, ws_sem, wr_sem,
           r_sem, out_sem, send_sem, recv_sem, xs_sem, xr_sem):
    me = lax.axis_index('terms')
    core = lax.rem(me, 2)
    xpos = lax.rem(lax.div(me, 2), 2)
    ypos = lax.div(me, 4)
    sib = me + 1 - 2 * core
    xn = me + 2 - 4 * xpos
    yn = me + 4 - 8 * ypos
    dg = yn + 2 - 4 * xpos
    sx = xn + 1 - 2 * core
    sy = yn + 1 - 2 * core
    sd = dg + 1 - 2 * core
    others = (sib, xn, sx, yn, sy, dg, sd)

    def rows(dev):
        return pl.ds(pl.multiple_of(dev * ROWS, 16), ROWS)

    def lanes(c):
        return pl.ds(pl.multiple_of(c * LANES, LANES), LANES)

    def remote(src, dst, ssem, rsem, target):
        return pltpu.make_async_remote_copy(src, dst, ssem, rsem, device_id=(target,), device_id_type=MESH)

    v_kinds = ((0, 4, me, xn, xn), (0, 4, me, yn, yn), (0, 4, me, sib, sib), (0, 2, xn, yn, dg), (2, 2, yn, xn, dg),
               (0, 4, xn, sib, sx), (0, 4, yn, sib, sy), (0, 4, dg, sib, sd))
    NV = len(v_kinds)

    def v_part(first, count, origin, c, g):
        return vbuf.at[c, pl.ds(4 * g + first, count), rows(origin), :]

    def v_sem(c, g, kind):
        return recv_sem.at[c * (NV * NKG) + g * NV + kind]

    def v_send(c, g, kind):
        first, count, origin, target, _ = v_kinds[kind]
        part = v_part(first, count, origin, c, g)
        remote(part, part, send_sem.at[kind], v_sem(c, g, kind), target).start()

    def v_landed(c, g, kind):
        first, count, _, target, origin = v_kinds[kind]
        part = v_part(first, count, origin, c, g)
        remote(part, part, send_sem.at[kind], v_sem(c, g, kind), target).wait_recv()

    def v_sent(kind):
        first, count, origin, target, _ = v_kinds[kind]
        part = vbuf.at[:, pl.ds(0, 4 * count), rows(origin), :]
        remote(part, part, send_sem.at[kind], recv_sem.at[kind], target).wait_send()

    def send_own(c, g):
        for kind in (0, 1, 2):
            v_send(c, g, kind)

    def relay_xy(c, g):
        v_landed(c, g, 0)
        v_send(c, g, 3)
        v_send(c, g, 5)
        v_landed(c, g, 1)
        v_send(c, g, 4)
        v_send(c, g, 6)

    def relay_diag(c, g):
        v_landed(c, g, 3)
        v_landed(c, g, 4)
        v_send(c, g, 7)

    def arrived(c, g):
        for kind in (2, 5, 6, 7):
            v_landed(c, g, kind)

    LO, HI, ALL = (0, 1), (1, 1), (0, 2)
    r_kinds = ((LO, me, xn, xn), (HI, me, xn, xn), (HI, me, yn, yn), (LO, me, yn, yn), (ALL, me, sib, sib),
               (LO, xn, yn, dg), (HI, yn, xn, dg), (ALL, xn, sib, sx), (ALL, yn, sib, sy), (ALL, dg, sib, sd))
    NR = len(r_kinds)

    def r_part(half, origin, c):
        return rall_h.at[pl.ds(2 * origin + half[0], half[1]), :, lanes(c)]

    def r_send(c, kind):
        half, origin, target, _ = r_kinds[kind]
        dst = r_part(half, origin, c)
        src = right_h.at[pl.ds(half[0], half[1]), :, lanes(c)] if kind < 5 else dst
        remote(src, dst, send_sem.at[kind], recv_sem.at[c * NR + kind], target).start()

    def r_landed(c, kind):
        half, _, target, origin = r_kinds[kind]
        part = r_part(half, origin, c)
        remote(part, part, send_sem.at[kind], recv_sem.at[c * NR + kind], target).wait_recv()

    def r_sent(kind):
        half, origin, target, _ = r_kinds[kind]
        part = rall_h.at[pl.ds(2 * origin + half[0], half[1])]
        remote(part, part, send_sem.at[kind], recv_sem.at[kind], target).wait_send()

    def left_copy(n):
        return remote(left_h.at[:, rows(others[n]), :], left.at[pl.ds(2 * me, 2)], ls_sem.at[n], lr_sem.at[n], others[n])

    def left_landed(n):
        part = left.at[pl.ds(2 * others[n], 2)]
        remote(part, part, ls_sem.at[n], lr_sem.at[n], others[n]).wait_recv()

    def pair_copy(n):
        return remote(pair_h, wall.at[pl.ds(2 * me, 2)], ws_sem.at[n], wr_sem.at[n], others[n])

    def pair_landed(n):
        part = wall.at[pl.ds(2 * others[n], 2)]
        remote(part, part, ws_sem.at[n], wr_sem.at[n], others[n]).wait_recv()

    def psi_copy(n):
        c, p, slot = lax.div(n, NP), lax.rem(n, NP), lax.rem(n, SLOTS)
        return pltpu.make_async_copy(psi_h.at[:, lax.div(p, 4), lax.rem(p, 4), lanes(c)], sig.at[:, lanes(slot)],
                                     psi_sem.at[slot])

    def vector_out(j):
        return [pltpu.make_async_copy(vec.at[pl.ds(p * ROWS, ROWS), :], kry_h.at[j, :, p // 4, p % 4, :],
                                      out_sem.at[p]) for p in range(NP)]

    def fold(x):
        return jnp.sum(x.reshape(-1, 8, LANES), axis=0)

    def exchange_start(par):
        exch[par, me] = mine[...]
        copies = [remote(mine, exch.at[par, me], xs_sem.at[n], xr_sem.at[par, n], others[n]) for n in range(NDEV - 1)]
        for cp in copies:
            cp.start()
        return copies

    def exchange_wait(par, copies):
        for n in range(NDEV - 1):
            remote(mine, exch.at[par, others[n]], xs_sem.at[n], xr_sem.at[par, n], others[n]).wait_recv()
        for cp in copies:
            cp.wait_send()

    barrier = pltpu.get_barrier_semaphore()
    for n in range(NDEV - 1):
        pl.semaphore_signal(barrier, inc=1, device_id=(others[n],), device_id_type=MESH)
    slab = [pltpu.make_async_copy(psi_h.at[rows(me), p // 4, p % 4, :], vec.at[pl.ds(p * ROWS, ROWS), :],
                                  slab_sem.at[p]) for p in range(NP)]
    for cp in slab:
        cp.start()
    own = [pltpu.make_async_copy(pair_h, wall.at[pl.ds(2 * me, 2)], own_sem.at[0]),
           pltpu.make_async_copy(left_h.at[:, rows(me), :], left.at[pl.ds(2 * me, 2)], own_sem.at[1])]
    for cp in own:
        cp.start()
    rest = [(h, c, rblk.at[(h * NCH + c) // KG, (h * NCH + c) % KG]) for h in range(2) for c in range(NCH)]
    take = [pltpu.make_async_copy(right_h.at[h, :, lanes(c)], at, rest_sem.at[n]) for n, (h, c, at) in enumerate(rest)]
    place_own = [pltpu.make_async_copy(at, rall_h.at[2 * me + h, :, lanes(c)], rest_sem.at[n])
                 for n, (h, c, at) in enumerate(rest)]
    for cp in take:
        cp.start()
    for n in range(SLOTS):
        psi_copy(n).start()
    zero = jnp.zeros((8, LANES), jnp.float32)
    for cp in slab:
        cp.wait()

    def squares(i, acc):
        at = pl.ds(pl.multiple_of(i * LANES, LANES), LANES)
        for c in range(NCH):
            x = vec[at, c * LANES:(c + 1) * LANES]
            acc = acc + fold(x * x)
        return acc

    mine[...] = jnp.full((8, LANES), jnp.sum(lax.fori_loop(0, SLOTS, squares, zero, unroll=2)))
    with jax.named_scope('barrier'):
        pl.semaphore_wait(barrier, NDEV - 1)
    copies = exchange_start(1)
    for n in range(NDEV - 1):
        pair_copy(n).start()
    for n in range(5):
        left_copy(n).start()

    def r_own(c):
        for kind in (4, 0, 2, 1, 3):
            r_send(c, kind)

    def operators_out(c, carry):
        r_own(c)
        return carry

    lax.fori_loop(0, 5, operators_out, 0)
    for n in (5, 6):
        left_copy(n).start()
    lax.fori_loop(5, NCH, operators_out, 0)
    for cp in take:
        cp.wait()
    for cp in place_own:
        cp.start()
    with jax.named_scope('exch0'):
        exchange_wait(1, copies)
    total = exch[1, 0]
    for d in range(1, NDEV):
        total = total + exch[1, d]
    scale[...] = 1.0 / jnp.sqrt(total * (1.0 / ELEMS))

    def normalise(i, carry):
        at = pl.ds(pl.multiple_of(i * LANES, LANES), LANES)
        for c in range(NCH):
            cs = slice(c * LANES, (c + 1) * LANES)
            vec[at, cs] = vec[at, cs] * scale[0:1, :]
        return carry

    lax.fori_loop(0, SLOTS, normalise, 0, unroll=2)
    for cp in vector_out(0):
        cp.start()

    for n in range(NDEV - 1):
        pair_landed(n)
    for cp in own:
        cp.wait()
    spread = (lax.div(lax.broadcasted_iota(jnp.int32, (256, 16), 0), 16)
              == lax.broadcasted_iota(jnp.int32, (256, 16), 1)).astype(jnp.float32).astype(jnp.bfloat16)
    same = (lax.rem(lax.broadcasted_iota(jnp.int32, (256, 256), 0), 16)
            == lax.rem(lax.broadcasted_iota(jnp.int32, (256, 256), 1), 16))

    def piece(n):
        vbuf[lax.div(n, NP), lax.rem(n, NP)] = (
            sig[:, lanes(lax.rem(n, SLOTS))] * scale[0:1, :]).astype(jnp.bfloat16)

    def opening_pieces(k, carry):
        tall = jnp.dot(spread, wall[k], preferred_element_type=jnp.float32).astype(jnp.bfloat16)
        full = lax.dot_general(tall, spread, (((1,), (1,)), ((), ())), preferred_element_type=jnp.float32)
        kron[k] = jnp.where(same, full, 0.0).astype(jnp.bfloat16)
        for t in range(4):
            n = 4 * k + t
            psi_copy(n).wait()
            piece(n)
            psi_copy(n + SLOTS).start()
        return carry

    with jax.named_scope('convert'):
        lax.fori_loop(0, TERMS, opening_pieces, 0)
    left_landed(0)
    with jax.named_scope('ownwait'):
        for cp in place_own:
            cp.wait()

    chip = lax.div(me, 2)

    def group(rel):
        return chip + lax.rem(rel, 2) * (1 - 2 * xpos) + lax.div(rel, 2) * (2 - 4 * ypos)

    def place(j, u):
        later = lax.div(j + STEPS - 1, STEPS)
        t = lax.div(u, NCH)
        mid, last = lax.div(t * (3 - t), 2), lax.div(t, 3)
        rel0 = mid * (1 + lax.rem(u + 1, 2)) + last * 3
        c0 = (1 - mid - last) * u + mid * lax.div(u - NCH, 2) + last * (u - 3 * NCH)
        c = later * lax.div(u, NKG) + (1 - later) * c0
        rel = later * lax.rem(u, NKG) + (1 - later) * rel0
        return c, rel, group(rel)

    def fetch_start(j, u, slot):
        c, _, kg = place(j, u)
        pltpu.make_async_copy(rall_h.at[pl.ds(kg * KG, KG), :, lanes(c)], rblk.at[slot], r_sem.at[slot]).start()

    def fetch_wait(slot):
        pltpu.make_async_copy(rall_h.at[pl.ds(0, KG), :, lanes(0)], rblk.at[slot], r_sem.at[slot]).wait()

    def stage_left(j, s, g):
        for i in range(NKG):
            c, _, kg = place(j, NKG * s + i)
            rhs = jnp.concatenate([vbuf[c, 4 * g + t] for t in range(4)], axis=1)
            lhs = left[pl.ds(kg * KG, KG)].reshape(KG * ROWS, BOND)
            o = jnp.dot(lhs, rhs, preferred_element_type=jnp.float32).astype(jnp.bfloat16)
            for t in range(4):
                ubuf[4 * g + t, i * KG * ROWS:(i + 1) * KG * ROWS, :] = o[:, t * LANES:(t + 1) * LANES]

    def stage_pair(j, s):
        for i in range(NKG):
            _, _, kg = place(j, NKG * s + i)
            for k in range(KG):
                row, at = (i * KG + k) * ROWS, k * LANES
                rhs = jnp.concatenate([ubuf[:, row + g * 16:row + (g + 1) * 16, :].reshape(256, LANES)
                                       for g in range(ROWS // 16)], axis=1)
                o = jnp.dot(kron[kg * KG + k], rhs, preferred_element_type=jnp.float32).astype(jnp.bfloat16)
                for g in range(ROWS // 16):
                    for q in range(NP):
                        zbuf[i, q * ROWS + g * 16:q * ROWS + (g + 1) * 16, at:at + LANES] = (
                            o[q * 16:(q + 1) * 16, g * LANES:(g + 1) * LANES])

    def stage_right(blocks, part):
        n0, n1 = NS[part][0] * LANES, NS[part][1] * LANES
        lhs = jnp.concatenate([rblk[slot, k] for _, slot in blocks for k in range(KG)], axis=1)
        rhs = jnp.concatenate([zbuf[i, n0:n1, :] for i, _ in blocks], axis=1)
        sig[:, n0:n1] += lax.dot_general(lhs, rhs, (((1,), (1,)), ((), ())), preferred_element_type=jnp.float32)

    def one_step(j, carry):
        beta_prev, cross = carry

        def r_before(q):
            for at, group in ((NKG, (1, 2)), (2 * NKG, (3, 4)), (5 * NKG, (5, 6))):
                @pl.when(q == at)
                def _(group=group):
                    for n in group:
                        left_landed(n)

            @pl.when((q >= 8) & (q < 8 + 2 * NCH) & (lax.rem(q, 2) == 0))
            def _():
                c = lax.div(q - 8, 2)
                for kind in (0, 2, 1, 3):
                    r_landed(c, kind)
                for kind in (5, 6, 7, 8):
                    r_send(c, kind)

            @pl.when(q >= 22)
            def _():
                c = q - 22
                r_landed(c, 5)
                r_landed(c, 6)
                r_send(c, 9)

        def fetch(u, slot=None):
            @pl.when(j == 0)
            def _():
                @pl.when(u < NCH)
                def _():
                    r_landed(u, 4)

                for odd, kind in ((1, 7), (0, 8)):
                    @pl.when((u >= NCH) & (u < 3 * NCH) & (lax.rem(u, 2) == odd))
                    def _(kind=kind):
                        r_landed(lax.div(u - NCH, 2), kind)

                @pl.when(u >= 3 * NCH)
                def _():
                    r_landed(u - 3 * NCH, 9)

            fetch_start(j, u, lax.rem(u, NKG) if slot is None else slot)

        def opening(g, carry):
            with jax.named_scope('first'):
                near, own = g + 1, g + 3
                relay_xy(lax.div(near, NKG), lax.rem(near, NKG))
                send_own(lax.div(own, NKG), lax.rem(own, NKG))
                relay_diag(0, g)
                arrived(0, g)
            with jax.named_scope('L'):
                stage_left(j, 0, g)
            return carry

        def opening_zero(g, carry):
            each = 12
            for t in range(each):
                psi_copy(4 * NP + each * g + t).wait()
            for t in range(each):
                piece(4 * NP + each * g + t)
            for t in range(each):
                n = 4 * NP + each * g + t + SLOTS

                @pl.when(n < NP * NCH)
                def _():
                    psi_copy(n).start()
            stage_left(j, 0, g)
            return carry

        @pl.when(j == 0)
        def _():
            with jax.named_scope('L0'):
                lax.fori_loop(0, NKG, opening_zero, 0)
                sig[...] = jnp.zeros((BOND, SLAB), jnp.float32)

        @pl.when(j > 0)
        def _():
            relay_xy(0, 0)
            send_own(0, 2)
            lax.fori_loop(0, NKG, opening, 0)
            with jax.named_scope('first3'):
                relay_xy(1, 1)
                send_own(1, 3)
                relay_diag(1, 0)
        for u in range(3):
            fetch(u)
        with jax.named_scope('W'):
            stage_pair(j, 0)

        def chunk(s, carry):
            def unit(g, carry):
                with jax.named_scope('before'):
                    @pl.when(j == 0)
                    def _():
                        r_before(NKG * s + g)

                    @pl.when(j > 0)
                    def _():
                        relay_diag(s, g + 1)

                        @pl.when(NKG * s + g < UNITS - 2)
                        def _():
                            ahead = g + 2
                            relay_xy(s + lax.div(ahead, NKG), lax.rem(ahead, NKG))

                        @pl.when(s < NCH - 1)
                        def _():
                            send_own(s + 1, g)

                        arrived(s, g)
                with jax.named_scope('RL'):
                    fetch_wait(g)
                    stage_left(j, s, g)
                    for part in range(len(NS)):
                        stage_right(((g, g),), part)
                with jax.named_scope('after'):
                    fetch(NKG * s + g - 1)
                return carry

            lax.fori_loop(0, NKG - 1, unit, 0)
            with jax.named_scope('before'):
                @pl.when(j == 0)
                def _():
                    r_before(NKG * s + NKG - 1)

                @pl.when(j > 0)
                def _():
                    @pl.when(s < NCH - 1)
                    def _():
                        relay_diag(s + 1, 0)
                        relay_xy(s + 1, 1)
                        send_own(s + 1, 3)

                    @pl.when(s == NCH - 1)
                    def _():
                        fetch_start(j, UNITS - 2, NKG - 2)
                        fetch_start(j, UNITS - 1, NKG)

                    arrived(s, NKG - 1)
            with jax.named_scope('LRW'):
                fetch_wait(NKG - 1)
                stage_left(j, s, NKG - 1)
                for part in range(len(NS)):
                    stage_right(((NKG - 1, NKG - 1),), part)
                stage_pair(j, s)
            with jax.named_scope('after'):
                @pl.when((j == 0) | (s < NCH - 1))
                def _():
                    fetch(NKG * s + 2)
            return carry

        lax.fori_loop(1, NCH, chunk, 0)

        @pl.when(j == 0)
        def _():
            r_before(UNITS)
            fetch(UNITS - 1, NKG)

        with jax.named_scope('sent'):
            @pl.when(j == 0)
            def _():
                for kind in range(NR):
                    r_sent(kind)
                for n in range(NDEV - 1):
                    left_copy(n).wait_send()
                    pair_copy(n).wait_send()

            @pl.when(j > 0)
            def _():
                for kind in range(NV):
                    v_sent(kind)

        with jax.named_scope('tail'):
            blocks = ((0, 0), (1, 1), (2, 2), (3, NKG))
            for _, slot in blocks:
                fetch_wait(slot)
            b_sum, v_sum = zero, zero
            for part in range(len(NS)):
                stage_right(blocks, part)
                for i in range(*NS[part]):
                    at = slice(i * LANES, (i + 1) * LANES)
                    for c in range(NCH):
                        cs = slice(c * LANES, (c + 1) * LANES)
                        s = sig[cs, at].T
                        v = vec[at, cs]
                        sig[cs, at] = s
                        b_sum = b_sum + fold(s * v)
                        v_sum = v_sum + fold(v * v)

        b_row = jnp.full((8, LANES), jnp.sum(b_sum))
        v_row = jnp.full((8, LANES), jnp.sum(v_sum))
        a_row = b_row + beta_prev * cross
        fit = jnp.where(v_row > 0, b_row / jnp.where(v_row > 0, v_row, 1.0), 0.0)
        fit_row = fit[0:1, :]

        def second(i, n_sum):
            at = pl.ds(pl.multiple_of(i * LANES, LANES), LANES)
            for c in range(NCH):
                cs = slice(c * LANES, (c + 1) * LANES)
                d = sig[cs, at] - fit_row * vec[at, cs]
                n_sum = n_sum + fold(d * d)
            return n_sum

        with jax.named_scope('pass2'):
            n_loc = jnp.sum(lax.fori_loop(0, SLOTS, second, zero, unroll=2))
        for cp in vector_out(j):
            cp.wait()

        row_id = lax.broadcasted_iota(jnp.int32, (8, LANES), 0)
        mine[...] = jnp.where(row_id == 0, a_row, jnp.where(
            row_id == 1, v_row, jnp.where(row_id == 2, fit, jnp.full((8, LANES), n_loc))))
        par = lax.rem(j, 2)
        with jax.named_scope('exch'):
            exchange_wait(par, exchange_start(par))
        total = exch[par, 0]
        for d in range(1, NDEV):
            total = total + exch[par, d]
        alpha = total[0:1, :] * (1.0 / ELEMS)
        square = jnp.zeros((1, LANES), jnp.float32)
        for d in range(NDEV):
            part = exch[par, d]
            gap = alpha - part[2:3, :]
            square = square + (part[3:4, :] + gap * gap * part[1:2, :])
        beta = jnp.sqrt(square * (1.0 / ELEMS))
        inv = 1.0 / beta
        ab_ref[j] = jnp.concatenate([alpha, beta] + [alpha] * 6, axis=0)

        def third(c, x_sum):
            cs = lanes(c)
            for i in range(SLOTS):
                at = slice(i * LANES, (i + 1) * LANES)
                v = vec[at, cs]
                n = (sig[cs, at] - alpha * v) * inv
                x_sum = x_sum + fold(v * n)
                vec[at, cs] = n
                low = n.astype(jnp.bfloat16)
                for t in range(8):
                    p, a = divmod(8 * i + t, ROWS // 16)
                    vbuf[c, p, pl.ds(pl.multiple_of(me * ROWS + 16 * a, 16), 16), :] = low[16 * t:16 * t + 16]
                sig[cs, at] = (v * -beta).T

            @pl.when((c < 2) & (j < STEPS - 1))
            def _():
                send_own(0, c)
            return x_sum

        with jax.named_scope('pass3'):
            x_sum = lax.fori_loop(0, NCH, third, zero)
        for cp in vector_out(j + 1):
            cp.start()
        return beta, jnp.full((8, LANES), jnp.sum(x_sum))

    lax.fori_loop(0, STEPS, one_step, (jnp.zeros((1, LANES), jnp.float32), zero))
    for cp in vector_out(STEPS):
        cp.wait()


def lanczos(psi, left, pair, right):
    dma = pltpu.SemaphoreType.DMA
    return pl.pallas_call(
        kernel,
        out_shape=(jax.ShapeDtypeStruct((STEPS + 1, ROWS, 4, 4, BOND), jnp.float32),
                   jax.ShapeDtypeStruct((TERMS, BOND, BOND), jnp.bfloat16),
                   jax.ShapeDtypeStruct((STEPS, 8, LANES), jnp.float32)),
        in_specs=[pl.BlockSpec(memory_space=pl.ANY)] * 4,
        out_specs=(pl.BlockSpec(memory_space=pl.ANY), pl.BlockSpec(memory_space=pl.ANY),
                   pl.BlockSpec(memory_space=pltpu.VMEM)),
        scratch_shapes=[
            pltpu.VMEM((NCH, NP, BOND, LANES), jnp.bfloat16),
            pltpu.VMEM((TERMS, ROWS, BOND), jnp.bfloat16),
            pltpu.VMEM((TERMS, 16, 16), jnp.bfloat16),
            pltpu.VMEM((TERMS, 256, 256), jnp.bfloat16),
            pltpu.VMEM((NKG + 1, KG, BOND, LANES), jnp.bfloat16),
            pltpu.VMEM((BOND, SLAB), jnp.float32),
            pltpu.VMEM((NP, TERMS * ROWS, LANES), jnp.bfloat16),
            pltpu.VMEM((NKG, SLAB, KG * LANES), jnp.bfloat16),
            pltpu.VMEM((SLAB, BOND), jnp.float32),
            pltpu.VMEM((8, LANES), jnp.float32),
            pltpu.VMEM((8, LANES), jnp.float32),
            pltpu.VMEM((2, NDEV, 8, LANES), jnp.float32),
            dma((NP,)), dma((SLOTS,)), dma((2,)), dma((2 * NCH,)), dma((NDEV - 1,)), dma((NDEV - 1,)), dma((NDEV - 1,)), dma((NDEV - 1,)),
            dma((NKG + 1,)), dma((NP,)), dma((10,)), dma((UNITS * 8,)), dma((NDEV - 1,)), dma((2, NDEV - 1)),
        ],
        compiler_params=pltpu.CompilerParams(collective_id=0, has_side_effects=True, vmem_limit_bytes=67043328),
    )(psi, left, pair, right)


def solution(mesh):
    def local_run(psi_init, left_env, op_pair, right_env):
        vectors, _, ab = lanczos(psi_init, left_env, op_pair, right_env)
        return vectors, ab[:, 0, 0], ab[:, 1, 0]

    return jax.shard_map(local_run, mesh=mesh, in_specs=(P(), P('terms'), P('terms'), P('terms')),
                         out_specs=(P(None, 'terms'), P(), P()), check_vma=False)
```

```python
import jax
import jax.numpy as jnp
from jax import lax
from jax.experimental import pallas as pl
from jax.experimental.pallas import tpu as pltpu
from jax.sharding import PartitionSpec as P

STEPS = 6
BOND = 896
NP = 16
TERMS = 16
NDEV = 8
ROWS = BOND // NDEV
LANES = 128
NCH = BOND // LANES
KG = 4
NKG = TERMS // KG
UNITS = NCH * NKG
SLAB = NP * ROWS
SLOTS = SLAB // LANES
TAIL = 96
ELEMS = BOND * NP * BOND
MESH = pl.DeviceIdType.MESH
NS = ((0, 4), (4, 8), (8, 12), (12, 14))


def kernel(psi_h, left_h, pair_h, right_h, kry_h, rall_h, ab_ref,
           vbuf, left, wall, kron, kmix, rblk, sig, ubuf, zbuf, vec, scale, mine, exch,
           slab_sem, psi_sem, own_sem, rest_sem, ls_sem, lr_sem, ws_sem, wr_sem,
           r_sem, out_sem, send_sem, recv_sem, xs_sem, xr_sem):
    me = lax.axis_index('terms')
    core = lax.rem(me, 2)
    xpos = lax.rem(lax.div(me, 2), 2)
    ypos = lax.div(me, 4)
    sib = me + 1 - 2 * core
    xn = me + 2 - 4 * xpos
    yn = me + 4 - 8 * ypos
    dg = yn + 2 - 4 * xpos
    sx = xn + 1 - 2 * core
    sy = yn + 1 - 2 * core
    sd = dg + 1 - 2 * core
    others = (sib, xn, sx, yn, sy, dg, sd)

    def rows(dev):
        return pl.ds(pl.multiple_of(dev * ROWS, 16), ROWS)

    def lanes(c):
        return pl.ds(pl.multiple_of(c * LANES, LANES), LANES)

    def remote(src, dst, ssem, rsem, target):
        return pltpu.make_async_remote_copy(src, dst, ssem, rsem, device_id=(target,), device_id_type=MESH)

    v_kinds = ((0, 4, me, xn, 0), (0, 4, me, yn, 1), (0, 4, me, sib, 3), (0, 2, xn, yn, 2), (2, 2, yn, xn, 2),
               (0, 4, xn, sib, 3), (0, 4, yn, sib, 3), (0, 4, dg, sib, 3))
    v_arrivals = (4, 4, 4, 16)
    NV = len(v_arrivals)

    def v_part(first, count, origin, c, g):
        return vbuf.at[c, pl.ds(4 * g + first, count), rows(origin), :]

    def v_sem(c, g, arrival):
        return recv_sem.at[c * (NV * NKG) + g * NV + arrival]

    def v_send(c, g, kind):
        first, count, origin, target, arrival = v_kinds[kind]
        part = v_part(first, count, origin, c, g)
        remote(part, part, send_sem.at[kind], v_sem(c, g, arrival), target).start()

    def v_landed(c, g, arrival):
        part = vbuf.at[c, pl.ds(0, v_arrivals[arrival]), rows(me), :]
        remote(part, part, send_sem.at[0], v_sem(c, g, arrival), sib).wait_recv()

    def v_sent(kind):
        first, count, origin, target, _ = v_kinds[kind]
        part = vbuf.at[:, pl.ds(0, 4 * count), rows(origin), :]
        remote(part, part, send_sem.at[kind], recv_sem.at[kind], target).wait_send()

    def send_own(c, g):
        for kind in (0, 1, 2):
            v_send(c, g, kind)

    def relay_xy(c, g):
        v_landed(c, g, 0)
        v_send(c, g, 3)
        v_send(c, g, 5)
        v_landed(c, g, 1)
        v_send(c, g, 4)
        v_send(c, g, 6)

    def relay_diag(c, g):
        v_landed(c, g, 2)
        v_send(c, g, 7)

    def arrived(c, g):
        v_landed(c, g, 3)

    LO, HI, ALL = (0, 1), (1, 1), (0, 2)
    r_kinds = ((LO, me, xn, xn), (HI, me, xn, xn), (HI, me, yn, yn), (LO, me, yn, yn), (ALL, me, sib, sib),
               (LO, xn, yn, dg), (HI, yn, xn, dg), (ALL, xn, sib, sx), (ALL, yn, sib, sy), (ALL, dg, sib, sd))
    NR = len(r_kinds)

    def r_part(half, origin, c):
        return rall_h.at[pl.ds(2 * origin + half[0], half[1]), :, lanes(c)]

    def r_send(c, kind):
        half, origin, target, _ = r_kinds[kind]
        dst = r_part(half, origin, c)
        src = right_h.at[pl.ds(half[0], half[1]), :, lanes(c)] if kind < 5 else dst
        remote(src, dst, send_sem.at[kind], recv_sem.at[c * NR + kind], target).start()

    def r_landed(c, kind):
        half, _, target, origin = r_kinds[kind]
        part = r_part(half, origin, c)
        remote(part, part, send_sem.at[kind], recv_sem.at[c * NR + kind], target).wait_recv()

    def r_sent(kind):
        half, origin, target, _ = r_kinds[kind]
        part = rall_h.at[pl.ds(2 * origin + half[0], half[1])]
        remote(part, part, send_sem.at[kind], recv_sem.at[kind], target).wait_send()

    def left_copy(n):
        return remote(left_h.at[:, rows(others[n]), :], left.at[pl.ds(2 * me, 2)], ls_sem.at[n], lr_sem.at[n], others[n])

    def regroup(dev):
        a, b = (left[2 * dev + h, TAIL:ROWS, :].astype(jnp.float32) for h in range(2))
        left[2 * dev, TAIL:ROWS, :] = jnp.concatenate([a[:8], b[:8]], axis=0).astype(jnp.bfloat16)
        left[2 * dev + 1, TAIL:ROWS, :] = jnp.concatenate([a[8:], b[8:]], axis=0).astype(jnp.bfloat16)

    def left_landed(n):
        part = left.at[pl.ds(2 * others[n], 2)]
        remote(part, part, ls_sem.at[n], lr_sem.at[n], others[n]).wait_recv()
        regroup(others[n])

    def pair_copy(n):
        return remote(pair_h, wall.at[pl.ds(2 * me, 2)], ws_sem.at[n], wr_sem.at[n], others[n])

    def pair_landed(n):
        part = wall.at[pl.ds(2 * others[n], 2)]
        remote(part, part, ws_sem.at[n], wr_sem.at[n], others[n]).wait_recv()

    def psi_copy(n):
        c, p, slot = lax.div(n, NP), lax.rem(n, NP), lax.rem(n, SLOTS)
        return pltpu.make_async_copy(psi_h.at[:, lax.div(p, 4), lax.rem(p, 4), lanes(c)], sig.at[:, lanes(slot)],
                                     psi_sem.at[slot])

    def vector_out(j):
        return [pltpu.make_async_copy(vec.at[pl.ds(p * ROWS, ROWS), :], kry_h.at[j, :, p // 4, p % 4, :],
                                      out_sem.at[p]) for p in range(NP)]

    def fold(x):
        return jnp.sum(x.reshape(-1, 8, LANES), axis=0)

    def exchange_start(par):
        exch[par, me] = mine[...]
        copies = [remote(mine, exch.at[par, me], xs_sem.at[n], xr_sem.at[par, n], others[n]) for n in range(NDEV - 1)]
        for cp in copies:
            cp.start()
        return copies

    def exchange_wait(par, copies):
        for n in range(NDEV - 1):
            remote(mine, exch.at[par, others[n]], xs_sem.at[n], xr_sem.at[par, n], others[n]).wait_recv()
        for cp in copies:
            cp.wait_send()

    barrier = pltpu.get_barrier_semaphore()
    for n in range(NDEV - 1):
        pl.semaphore_signal(barrier, inc=1, device_id=(others[n],), device_id_type=MESH)
    slab = [pltpu.make_async_copy(psi_h.at[rows(me), p // 4, p % 4, :], vec.at[pl.ds(p * ROWS, ROWS), :],
                                  slab_sem.at[p]) for p in range(NP)]
    for cp in slab:
        cp.start()
    own = [pltpu.make_async_copy(pair_h, wall.at[pl.ds(2 * me, 2)], own_sem.at[0]),
           pltpu.make_async_copy(left_h.at[:, rows(me), :], left.at[pl.ds(2 * me, 2)], own_sem.at[1])]
    for cp in own:
        cp.start()
    rest = [(h, c, rblk.at[(h * NCH + c) // KG, (h * NCH + c) % KG]) for h in range(2) for c in range(NCH)]
    take = [pltpu.make_async_copy(right_h.at[h, :, lanes(c)], at, rest_sem.at[n]) for n, (h, c, at) in enumerate(rest)]
    place_own = [pltpu.make_async_copy(at, rall_h.at[2 * me + h, :, lanes(c)], rest_sem.at[n])
                 for n, (h, c, at) in enumerate(rest)]
    for cp in take:
        cp.start()
    for n in range(SLOTS):
        psi_copy(n).start()
    zero = jnp.zeros((8, LANES), jnp.float32)
    with jax.named_scope('barrier'):
        pl.semaphore_wait(barrier, NDEV - 1)
    for n in (0, 1, 3):
        left_copy(n).start()
    for cp in slab:
        cp.wait()

    def squares(i, acc):
        at = pl.ds(pl.multiple_of(i * LANES, LANES), LANES)
        for c in range(NCH):
            x = vec[at, c * LANES:(c + 1) * LANES]
            acc = acc + fold(x * x)
        return acc

    mine[...] = jnp.full((8, LANES), jnp.sum(lax.fori_loop(0, SLOTS, squares, zero, unroll=2)))
    copies = exchange_start(1)
    for n in range(NDEV - 1):
        pair_copy(n).start()
    for n in (2, 4):
        left_copy(n).start()

    def r_own(c):
        for kind in (4, 0, 2, 1, 3):
            r_send(c, kind)

    def operators_out(c, carry):
        r_own(c)
        return carry

    lax.fori_loop(0, 5, operators_out, 0)
    for n in (5, 6):
        left_copy(n).start()
    lax.fori_loop(5, NCH, operators_out, 0)
    for cp in take:
        cp.wait()
    for cp in place_own:
        cp.start()
    with jax.named_scope('exch0'):
        exchange_wait(1, copies)
    total = exch[1, 0]
    for d in range(1, NDEV):
        total = total + exch[1, d]
    scale[...] = 1.0 / jnp.sqrt(total * (1.0 / ELEMS))

    def normalise(i, carry):
        at = pl.ds(pl.multiple_of(i * LANES, LANES), LANES)
        for c in range(NCH):
            cs = slice(c * LANES, (c + 1) * LANES)
            vec[at, cs] = vec[at, cs] * scale[0:1, :]
        return carry

    lax.fori_loop(0, SLOTS, normalise, 0, unroll=2)
    for cp in vector_out(0):
        cp.start()

    for n in range(NDEV - 1):
        pair_landed(n)
    for cp in own:
        cp.wait()
    spread = (lax.div(lax.broadcasted_iota(jnp.int32, (256, 16), 0), 16)
              == lax.broadcasted_iota(jnp.int32, (256, 16), 1)).astype(jnp.float32).astype(jnp.bfloat16)
    same = (lax.rem(lax.broadcasted_iota(jnp.int32, (256, 256), 0), 16)
            == lax.rem(lax.broadcasted_iota(jnp.int32, (256, 256), 1), 16))

    def piece(n):
        vbuf[lax.div(n, NP), lax.rem(n, NP)] = (
            sig[:, lanes(lax.rem(n, SLOTS))] * scale[0:1, :]).astype(jnp.bfloat16)

    def opening_pieces(k, carry):
        tall = jnp.dot(spread, wall[k], preferred_element_type=jnp.float32).astype(jnp.bfloat16)
        full = lax.dot_general(tall, spread, (((1,), (1,)), ((), ())), preferred_element_type=jnp.float32)
        kron[k] = jnp.where(same, full, 0.0).astype(jnp.bfloat16)
        for t in range(4):
            n = 4 * k + t
            psi_copy(n).wait()
            piece(n)
            psi_copy(n + SLOTS).start()
        return carry

    with jax.named_scope('convert'):
        lax.fori_loop(0, TERMS, opening_pieces, 0)
    left_landed(0)
    regroup(me)
    first_half = lax.rem(lax.broadcasted_iota(jnp.int32, (256, 256), 0), 16) < 8

    def mix(n, carry):
        kmix[n] = jnp.where(first_half, kron[2 * n].astype(jnp.float32),
                            kron[2 * n + 1].astype(jnp.float32)).astype(jnp.bfloat16)
        return carry

    lax.fori_loop(0, TERMS // 2, mix, 0)
    with jax.named_scope('ownwait'):
        for cp in place_own:
            cp.wait()

    chip = lax.div(me, 2)

    def group(rel):
        return chip + lax.rem(rel, 2) * (1 - 2 * xpos) + lax.div(rel, 2) * (2 - 4 * ypos)

    def place(j, u):
        later = lax.div(j + STEPS - 1, STEPS)
        t = lax.div(u, NCH)
        mid, last = lax.div(t * (3 - t), 2), lax.div(t, 3)
        rel0 = mid * (1 + lax.rem(u + 1, 2)) + last * 3
        c0 = (1 - mid - last) * u + mid * lax.div(u - NCH, 2) + last * (u - 3 * NCH)
        c = later * lax.div(u, NKG) + (1 - later) * c0
        rel = later * lax.rem(u, NKG) + (1 - later) * rel0
        return c, rel, group(rel)

    def fetch_start(j, u, slot):
        c, _, kg = place(j, u)
        pltpu.make_async_copy(rall_h.at[pl.ds(kg * KG, KG), :, lanes(c)], rblk.at[slot], r_sem.at[slot]).start()

    def fetch_wait(slot):
        pltpu.make_async_copy(rall_h.at[pl.ds(0, KG), :, lanes(0)], rblk.at[slot], r_sem.at[slot]).wait()

    def stage_left(j, s, g):
        for i in range(NKG):
            c, _, kg = place(j, NKG * s + i)
            rhs = jnp.concatenate([vbuf[c, 4 * g + t] for t in range(4)], axis=1)
            lhs = left[pl.ds(kg * KG, KG)].reshape(KG * ROWS, BOND)
            o = jnp.dot(lhs, rhs, preferred_element_type=jnp.float32).astype(jnp.bfloat16)
            for t in range(4):
                ubuf[4 * g + t, i * KG * ROWS:(i + 1) * KG * ROWS, :] = o[:, t * LANES:(t + 1) * LANES]

    def stage_pair(j, s):
        for i in range(NKG):
            _, _, kg = place(j, NKG * s + i)

            def columns(row):
                return ubuf[:, row:row + 16, :].reshape(256, LANES)

            for k in range(KG):
                row, at = (i * KG + k) * ROWS, k * LANES
                rhs = jnp.concatenate([columns(row + g * 16) for g in range(TAIL // 16)], axis=1)
                o = jnp.dot(kron[kg * KG + k], rhs, preferred_element_type=jnp.float32).astype(jnp.bfloat16)
                for g in range(TAIL // 16):
                    for q in range(NP):
                        zbuf[i, q * ROWS + g * 16:q * ROWS + (g + 1) * 16, at:at + LANES] = (
                            o[q * 16:(q + 1) * 16, g * LANES:(g + 1) * LANES])
            for n in range(KG // 2):
                row = (i * KG + 2 * n) * ROWS + TAIL
                rhs = jnp.concatenate([columns(row), columns(row + ROWS)], axis=1)
                o = jnp.dot(kmix[kg * (KG // 2) + n], rhs, preferred_element_type=jnp.float32)
                for h in range(2):
                    at = (2 * n + h) * LANES
                    for q in range(NP):
                        half = o[q * 16 + 8 * h:q * 16 + 8 * h + 8]
                        zbuf[i, q * ROWS + TAIL:(q + 1) * ROWS, at:at + LANES] = jnp.concatenate(
                            [half[:, :LANES], half[:, LANES:]], axis=0).astype(jnp.bfloat16)

    def stage_right(blocks, part):
        n0, n1 = NS[part][0] * LANES, NS[part][1] * LANES
        lhs = jnp.concatenate([rblk[slot, k] for _, slot in blocks for k in range(KG)], axis=1)
        rhs = jnp.concatenate([zbuf[i, n0:n1, :] for i, _ in blocks], axis=1)
        sig[:, n0:n1] += lax.dot_general(lhs, rhs, (((1,), (1,)), ((), ())), preferred_element_type=jnp.float32)

    def one_step(j, carry):
        beta_prev, cross = carry

        def r_before(q):
            for at, group in ((NKG, (1, 2)), (2 * NKG, (3, 4)), (5 * NKG, (5, 6))):
                @pl.when(q == at)
                def _(group=group):
                    for n in group:
                        left_landed(n)

            @pl.when((q >= 8) & (q < 8 + 2 * NCH) & (lax.rem(q, 2) == 0))
            def _():
                c = lax.div(q - 8, 2)
                for kind in (0, 2, 1, 3):
                    r_landed(c, kind)
                for kind in (5, 6, 7, 8):
                    r_send(c, kind)

            @pl.when(q >= 22)
            def _():
                c = q - 22
                r_landed(c, 5)
                r_landed(c, 6)
                r_send(c, 9)

        def fetch(u, slot=None):
            @pl.when(j == 0)
            def _():
                @pl.when(u < NCH)
                def _():
                    r_landed(u, 4)

                for odd, kind in ((1, 7), (0, 8)):
                    @pl.when((u >= NCH) & (u < 3 * NCH) & (lax.rem(u, 2) == odd))
                    def _(kind=kind):
                        r_landed(lax.div(u - NCH, 2), kind)

                @pl.when(u >= 3 * NCH)
                def _():
                    r_landed(u - 3 * NCH, 9)

            fetch_start(j, u, lax.rem(u, NKG) if slot is None else slot)

        def opening(g, carry):
            with jax.named_scope('first'):
                near, own = g + 1, g + 3
                relay_xy(lax.div(near, NKG), lax.rem(near, NKG))
                send_own(lax.div(own, NKG), lax.rem(own, NKG))
                relay_diag(0, g)
                arrived(0, g)
            with jax.named_scope('L'):
                stage_left(j, 0, g)
            return carry

        def opening_zero(g, carry):
            each = 12
            for t in range(each):
                psi_copy(4 * NP + each * g + t).wait()
            for t in range(each):
                piece(4 * NP + each * g + t)
            for t in range(each):
                n = 4 * NP + each * g + t + SLOTS

                @pl.when(n < NP * NCH)
                def _():
                    psi_copy(n).start()
            stage_left(j, 0, g)
            return carry

        @pl.when(j == 0)
        def _():
            with jax.named_scope('L0'):
                lax.fori_loop(0, NKG, opening_zero, 0)
                sig[...] = jnp.zeros((BOND, SLAB), jnp.float32)

        @pl.when(j > 0)
        def _():
            relay_xy(0, 0)
            send_own(0, 2)
            lax.fori_loop(0, NKG, opening, 0)
            with jax.named_scope('first3'):
                relay_xy(1, 1)
                send_own(1, 3)
                relay_diag(1, 0)
        for u in range(3):
            fetch(u)
        with jax.named_scope('W'):
            stage_pair(j, 0)

        def chunk(s, carry):
            def unit(g, carry):
                with jax.named_scope('before'):
                    @pl.when(j == 0)
                    def _():
                        r_before(NKG * s + g)

                    @pl.when(j > 0)
                    def _():
                        relay_diag(s, g + 1)

                        @pl.when(NKG * s + g < UNITS - 2)
                        def _():
                            ahead = g + 2
                            relay_xy(s + lax.div(ahead, NKG), lax.rem(ahead, NKG))

                        @pl.when(s < NCH - 1)
                        def _():
                            send_own(s + 1, g)

                        arrived(s, g)
                with jax.named_scope('RL'):
                    fetch_wait(g)
                    stage_left(j, s, g)
                    for part in range(len(NS)):
                        stage_right(((g, g),), part)
                with jax.named_scope('after'):
                    fetch(NKG * s + g - 1)
                return carry

            lax.fori_loop(0, NKG - 1, unit, 0)
            with jax.named_scope('before'):
                @pl.when(j == 0)
                def _():
                    r_before(NKG * s + NKG - 1)

                @pl.when(j > 0)
                def _():
                    @pl.when(s < NCH - 1)
                    def _():
                        relay_diag(s + 1, 0)
                        relay_xy(s + 1, 1)
                        send_own(s + 1, 3)

                    @pl.when(s == NCH - 1)
                    def _():
                        fetch_start(j, UNITS - 2, NKG - 2)
                        fetch_start(j, UNITS - 1, NKG)

                    arrived(s, NKG - 1)
            with jax.named_scope('LRW'):
                fetch_wait(NKG - 1)
                stage_left(j, s, NKG - 1)
                for part in range(len(NS)):
                    stage_right(((NKG - 1, NKG - 1),), part)
                stage_pair(j, s)
            with jax.named_scope('after'):
                @pl.when((j == 0) | (s < NCH - 1))
                def _():
                    fetch(NKG * s + 2)
            return carry

        lax.fori_loop(1, NCH, chunk, 0)

        @pl.when(j == 0)
        def _():
            r_before(UNITS)
            fetch(UNITS - 1, NKG)

        with jax.named_scope('sent'):
            @pl.when(j == 0)
            def _():
                for kind in range(NR):
                    r_sent(kind)
                for n in range(NDEV - 1):
                    left_copy(n).wait_send()
                    pair_copy(n).wait_send()

            @pl.when(j > 0)
            def _():
                for kind in range(len(v_kinds)):
                    v_sent(kind)

        with jax.named_scope('tail'):
            blocks = ((0, 0), (1, 1), (2, 2), (3, NKG))
            for _, slot in blocks:
                fetch_wait(slot)
            b_sum, v_sum = zero, zero
            for part in range(len(NS)):
                stage_right(blocks, part)
                for i in range(*NS[part]):
                    at = slice(i * LANES, (i + 1) * LANES)
                    for c in range(NCH):
                        cs = slice(c * LANES, (c + 1) * LANES)
                        s = sig[cs, at].T
                        v = vec[at, cs]
                        sig[cs, at] = s
                        b_sum = b_sum + fold(s * v)
                        v_sum = v_sum + fold(v * v)

        b_row = jnp.full((8, LANES), jnp.sum(b_sum))
        v_row = jnp.full((8, LANES), jnp.sum(v_sum))
        a_row = b_row + beta_prev * cross
        fit = jnp.where(v_row > 0, b_row / jnp.where(v_row > 0, v_row, 1.0), 0.0)
        fit_row = fit[0:1, :]

        def second(i, n_sum):
            at = pl.ds(pl.multiple_of(i * LANES, LANES), LANES)
            for c in range(NCH):
                cs = slice(c * LANES, (c + 1) * LANES)
                d = sig[cs, at] - fit_row * vec[at, cs]
                n_sum = n_sum + fold(d * d)
            return n_sum

        with jax.named_scope('pass2'):
            n_loc = jnp.sum(lax.fori_loop(0, SLOTS, second, zero, unroll=2))
        for cp in vector_out(j):
            cp.wait()

        row_id = lax.broadcasted_iota(jnp.int32, (8, LANES), 0)
        mine[...] = jnp.where(row_id == 0, a_row, jnp.where(
            row_id == 1, v_row, jnp.where(row_id == 2, fit, jnp.full((8, LANES), n_loc))))
        par = lax.rem(j, 2)
        with jax.named_scope('exch'):
            exchange_wait(par, exchange_start(par))
        total = exch[par, 0]
        for d in range(1, NDEV):
            total = total + exch[par, d]
        alpha = total[0:1, :] * (1.0 / ELEMS)
        square = jnp.zeros((1, LANES), jnp.float32)
        for d in range(NDEV):
            part = exch[par, d]
            gap = alpha - part[2:3, :]
            square = square + (part[3:4, :] + gap * gap * part[1:2, :])
        beta = jnp.sqrt(square * (1.0 / ELEMS))
        inv = 1.0 / beta
        ab_ref[j] = jnp.concatenate([alpha, beta] + [alpha] * 6, axis=0)

        def third(c, x_sum):
            cs = lanes(c)
            for i in range(SLOTS):
                at = slice(i * LANES, (i + 1) * LANES)
                v = vec[at, cs]
                n = (sig[cs, at] - alpha * v) * inv
                x_sum = x_sum + fold(v * n)
                vec[at, cs] = n
                low = n.astype(jnp.bfloat16)
                for t in range(8):
                    p, a = divmod(8 * i + t, ROWS // 16)
                    vbuf[c, p, pl.ds(pl.multiple_of(me * ROWS + 16 * a, 16), 16), :] = low[16 * t:16 * t + 16]
                sig[cs, at] = (v * -beta).T

            @pl.when((c < 2) & (j < STEPS - 1))
            def _():
                send_own(0, c)
            return x_sum

        with jax.named_scope('pass3'):
            x_sum = lax.fori_loop(0, NCH, third, zero)
        for cp in vector_out(j + 1):
            cp.start()
        return beta, jnp.full((8, LANES), jnp.sum(x_sum))

    lax.fori_loop(0, STEPS, one_step, (jnp.zeros((1, LANES), jnp.float32), zero))
    for cp in vector_out(STEPS):
        cp.wait()


def lanczos(psi, left, pair, right):
    dma = pltpu.SemaphoreType.DMA
    return pl.pallas_call(
        kernel,
        out_shape=(jax.ShapeDtypeStruct((STEPS + 1, ROWS, 4, 4, BOND), jnp.float32),
                   jax.ShapeDtypeStruct((TERMS, BOND, BOND), jnp.bfloat16),
                   jax.ShapeDtypeStruct((STEPS, 8, LANES), jnp.float32)),
        in_specs=[pl.BlockSpec(memory_space=pl.ANY)] * 4,
        out_specs=(pl.BlockSpec(memory_space=pl.ANY), pl.BlockSpec(memory_space=pl.ANY),
                   pl.BlockSpec(memory_space=pltpu.VMEM)),
        scratch_shapes=[
            pltpu.VMEM((NCH, NP, BOND, LANES), jnp.bfloat16),
            pltpu.VMEM((TERMS, ROWS, BOND), jnp.bfloat16),
            pltpu.VMEM((TERMS, 16, 16), jnp.bfloat16),
            pltpu.VMEM((TERMS, 256, 256), jnp.bfloat16),
            pltpu.VMEM((TERMS // 2, 256, 256), jnp.bfloat16),
            pltpu.VMEM((NKG + 1, KG, BOND, LANES), jnp.bfloat16),
            pltpu.VMEM((BOND, SLAB), jnp.float32),
            pltpu.VMEM((NP, TERMS * ROWS, LANES), jnp.bfloat16),
            pltpu.VMEM((NKG, SLAB, KG * LANES), jnp.bfloat16),
            pltpu.VMEM((SLAB, BOND), jnp.float32),
            pltpu.VMEM((8, LANES), jnp.float32),
            pltpu.VMEM((8, LANES), jnp.float32),
            pltpu.VMEM((2, NDEV, 8, LANES), jnp.float32),
            dma((NP,)), dma((SLOTS,)), dma((2,)), dma((2 * NCH,)), dma((NDEV - 1,)), dma((NDEV - 1,)), dma((NDEV - 1,)), dma((NDEV - 1,)),
            dma((NKG + 1,)), dma((NP,)), dma((10,)), dma((UNITS * 4,)), dma((NDEV - 1,)), dma((2, NDEV - 1)),
        ],
        compiler_params=pltpu.CompilerParams(collective_id=0, has_side_effects=True, vmem_limit_bytes=67043328),
    )(psi, left, pair, right)


def solution(mesh):
    def local_run(psi_init, left_env, op_pair, right_env):
        vectors, _, ab = lanczos(psi_init, left_env, op_pair, right_env)
        return vectors, ab[:, 0, 0], ab[:, 1, 0]

    return jax.shard_map(local_run, mesh=mesh, in_specs=(P(), P('terms'), P('terms'), P('terms')),
                         out_specs=(P(None, 'terms'), P(), P()), check_vma=False)
```

```python
import jax
import jax.numpy as jnp
from jax import lax
from jax.experimental import pallas as pl
from jax.experimental.pallas import tpu as pltpu
from jax.sharding import PartitionSpec as P

STEPS = 6
BOND = 896
NP = 16
TERMS = 16
NDEV = 8
ROWS = BOND // NDEV
LANES = 128
NCH = BOND // LANES
KG = 4
NKG = TERMS // KG
UNITS = NCH * NKG
SLAB = NP * ROWS
SLOTS = SLAB // LANES
TAIL = 96
ELEMS = BOND * NP * BOND
MESH = pl.DeviceIdType.MESH
NS = ((0, 4), (4, 8), (8, 12), (12, 14))


def kernel(psi_h, left_h, pair_h, right_h, kry_h, rall_h, ab_ref,
           vbuf, left, wall, kron, kmix, rblk, sig, ubuf, zbuf, vec, scale, mine, exch,
           slab_sem, psi_sem, own_sem, rest_sem, ls_sem, lr_sem, ws_sem, wr_sem,
           r_sem, out_sem, send_sem, recv_sem, xs_sem, xr_sem):
    me = lax.axis_index('terms')
    core = lax.rem(me, 2)
    xpos = lax.rem(lax.div(me, 2), 2)
    ypos = lax.div(me, 4)
    sib = me + 1 - 2 * core
    xn = me + 2 - 4 * xpos
    yn = me + 4 - 8 * ypos
    dg = yn + 2 - 4 * xpos
    sx = xn + 1 - 2 * core
    sy = yn + 1 - 2 * core
    sd = dg + 1 - 2 * core
    others = (sib, xn, sx, yn, sy, dg, sd)

    def rows(dev):
        return pl.ds(pl.multiple_of(dev * ROWS, 16), ROWS)

    def lanes(c):
        return pl.ds(pl.multiple_of(c * LANES, LANES), LANES)

    def remote(src, dst, ssem, rsem, target):
        return pltpu.make_async_remote_copy(src, dst, ssem, rsem, device_id=(target,), device_id_type=MESH)

    v_kinds = ((0, 4, me, xn, 0), (0, 4, me, yn, 1), (0, 4, me, sib, 3), (0, 2, xn, yn, 2), (2, 2, yn, xn, 2),
               (0, 4, xn, sib, 3), (0, 4, yn, sib, 3), (0, 4, dg, sib, 3))
    v_arrivals = (4, 4, 4, 16)
    NV = len(v_arrivals)

    def v_part(first, count, origin, c, g):
        return vbuf.at[c, pl.ds(4 * g + first, count), rows(origin), :]

    def v_sem(c, g, arrival):
        return recv_sem.at[c * (NV * NKG) + g * NV + arrival]

    def v_send(c, g, kind):
        first, count, origin, target, arrival = v_kinds[kind]
        part = v_part(first, count, origin, c, g)
        remote(part, part, send_sem.at[kind], v_sem(c, g, arrival), target).start()

    def v_landed(c, g, arrival):
        part = vbuf.at[c, pl.ds(0, v_arrivals[arrival]), rows(me), :]
        remote(part, part, send_sem.at[0], v_sem(c, g, arrival), sib).wait_recv()

    def v_sent(kind):
        first, count, origin, target, _ = v_kinds[kind]
        part = vbuf.at[:, pl.ds(0, 4 * count), rows(origin), :]
        remote(part, part, send_sem.at[kind], recv_sem.at[kind], target).wait_send()

    def send_own(c, g):
        for kind in (0, 1, 2):
            v_send(c, g, kind)

    def relay_xy(c, g):
        v_landed(c, g, 0)
        v_send(c, g, 3)
        v_send(c, g, 5)
        v_landed(c, g, 1)
        v_send(c, g, 4)
        v_send(c, g, 6)

    def relay_diag(c, g):
        v_landed(c, g, 2)
        v_send(c, g, 7)

    def arrived(c, g):
        v_landed(c, g, 3)

    LO, HI, ALL = (0, 1), (1, 1), (0, 2)
    r_kinds = ((LO, me, xn, xn), (HI, me, xn, xn), (HI, me, yn, yn), (LO, me, yn, yn), (ALL, me, sib, sib),
               (LO, xn, yn, dg), (HI, yn, xn, dg), (ALL, xn, sib, sx), (ALL, yn, sib, sy), (ALL, dg, sib, sd))
    NR = len(r_kinds)

    def r_part(half, origin, c):
        return rall_h.at[pl.ds(2 * origin + half[0], half[1]), :, lanes(c)]

    def r_send(c, kind):
        half, origin, target, _ = r_kinds[kind]
        dst = r_part(half, origin, c)
        src = right_h.at[pl.ds(half[0], half[1]), :, lanes(c)] if kind < 5 else dst
        remote(src, dst, send_sem.at[kind], recv_sem.at[c * NR + kind], target).start()

    def r_landed(c, kind):
        half, _, target, origin = r_kinds[kind]
        part = r_part(half, origin, c)
        remote(part, part, send_sem.at[kind], recv_sem.at[c * NR + kind], target).wait_recv()

    def r_sent(kind):
        half, origin, target, _ = r_kinds[kind]
        part = rall_h.at[pl.ds(2 * origin + half[0], half[1])]
        remote(part, part, send_sem.at[kind], recv_sem.at[kind], target).wait_send()

    def left_copy(n, h):
        return remote(left_h.at[h, rows(others[n]), :], left.at[2 * me + h], ls_sem.at[2 * n + h], lr_sem.at[2 * n + h],
                      others[n])

    def regroup(dev):
        a, b = (left[2 * dev + h, TAIL:ROWS, :].astype(jnp.float32) for h in range(2))
        left[2 * dev, TAIL:ROWS, :] = jnp.concatenate([a[:8], b[:8]], axis=0).astype(jnp.bfloat16)
        left[2 * dev + 1, TAIL:ROWS, :] = jnp.concatenate([a[8:], b[8:]], axis=0).astype(jnp.bfloat16)

    def left_landed(n):
        for h in range(2):
            part = left.at[2 * others[n] + h]
            remote(part, part, ls_sem.at[2 * n + h], lr_sem.at[2 * n + h], others[n]).wait_recv()
        regroup(others[n])

    def pair_copy(n):
        return remote(pair_h, wall.at[pl.ds(2 * me, 2)], ws_sem.at[n], wr_sem.at[n], others[n])

    def pair_landed(n):
        part = wall.at[pl.ds(2 * others[n], 2)]
        remote(part, part, ws_sem.at[n], wr_sem.at[n], others[n]).wait_recv()

    def psi_copy(n):
        c, p, slot = lax.div(n, NP), lax.rem(n, NP), lax.rem(n, SLOTS)
        return pltpu.make_async_copy(psi_h.at[:, lax.div(p, 4), lax.rem(p, 4), lanes(c)], sig.at[:, lanes(slot)],
                                     psi_sem.at[slot])

    def vector_out(j):
        return [pltpu.make_async_copy(vec.at[pl.ds(p * ROWS, ROWS), :], kry_h.at[j, :, p // 4, p % 4, :],
                                      out_sem.at[p]) for p in range(NP)]

    def chunk_out(j, c):
        for p in range(NP):
            pltpu.make_async_copy(vec.at[pl.ds(p * ROWS, ROWS), lanes(c)], kry_h.at[j, :, p // 4, p % 4, lanes(c)],
                                  out_sem.at[p]).start()

    def fold(x):
        return jnp.sum(x.reshape(-1, 8, LANES), axis=0)

    def exchange_start(par):
        exch[par, me] = mine[...]
        copies = [remote(mine, exch.at[par, me], xs_sem.at[n], xr_sem.at[par, n], others[n]) for n in range(NDEV - 1)]
        for cp in copies:
            cp.start()
        return copies

    def exchange_wait(par, copies):
        for n in range(NDEV - 1):
            remote(mine, exch.at[par, others[n]], xs_sem.at[n], xr_sem.at[par, n], others[n]).wait_recv()
        for cp in copies:
            cp.wait_send()

    barrier = pltpu.get_barrier_semaphore()
    for n in range(NDEV - 1):
        pl.semaphore_signal(barrier, inc=1, device_id=(others[n],), device_id_type=MESH)
    slab = [pltpu.make_async_copy(psi_h.at[rows(me), p // 4, p % 4, :], vec.at[pl.ds(p * ROWS, ROWS), :],
                                  slab_sem.at[p]) for p in range(NP)]
    for cp in slab:
        cp.start()
    own = [pltpu.make_async_copy(pair_h, wall.at[pl.ds(2 * me, 2)], own_sem.at[0]),
           pltpu.make_async_copy(left_h.at[:, rows(me), :], left.at[pl.ds(2 * me, 2)], own_sem.at[1])]
    for cp in own:
        cp.start()
    rest = [(h, c, rblk.at[(h * NCH + c) // KG, (h * NCH + c) % KG]) for h in range(2) for c in range(NCH)]
    take = [pltpu.make_async_copy(right_h.at[h, :, lanes(c)], at, rest_sem.at[n]) for n, (h, c, at) in enumerate(rest)]
    place_own = [pltpu.make_async_copy(at, rall_h.at[2 * me + h, :, lanes(c)], rest_sem.at[n])
                 for n, (h, c, at) in enumerate(rest)]
    for cp in take:
        cp.start()
    for n in range(SLOTS):
        psi_copy(n).start()
    zero = jnp.zeros((8, LANES), jnp.float32)
    with jax.named_scope('barrier'):
        pl.semaphore_wait(barrier, NDEV - 1)
    for n, h in ((1, 0), (3, 0), (0, 0), (0, 1)):
        left_copy(n, h).start()
    for cp in slab:
        cp.wait()

    def squares(i, acc):
        at = pl.ds(pl.multiple_of(i * LANES, LANES), LANES)
        for c in range(NCH):
            x = vec[at, c * LANES:(c + 1) * LANES]
            acc = acc + fold(x * x)
        return acc

    mine[...] = jnp.full((8, LANES), jnp.sum(lax.fori_loop(0, SLOTS, squares, zero, unroll=2)))
    copies = exchange_start(1)
    for n in range(NDEV - 1):
        pair_copy(n).start()
    for n, h in ((1, 1), (3, 1), (2, 0), (4, 0), (2, 1), (4, 1)):
        left_copy(n, h).start()

    def r_own(c):
        for kind in (4, 0, 2, 1, 3):
            r_send(c, kind)

    def operators_out(c, carry):
        r_own(c)
        return carry

    lax.fori_loop(0, 5, operators_out, 0)
    for n in (5, 6):
        for h in range(2):
            left_copy(n, h).start()
    lax.fori_loop(5, NCH, operators_out, 0)
    for cp in take:
        cp.wait()
    for cp in place_own:
        cp.start()
    with jax.named_scope('exch0'):
        exchange_wait(1, copies)
    total = exch[1, 0]
    for d in range(1, NDEV):
        total = total + exch[1, d]
    scale[...] = 1.0 / jnp.sqrt(total * (1.0 / ELEMS))

    def normalise(i, carry):
        at = pl.ds(pl.multiple_of(i * LANES, LANES), LANES)
        for c in range(NCH):
            cs = slice(c * LANES, (c + 1) * LANES)
            vec[at, cs] = vec[at, cs] * scale[0:1, :]
        return carry

    lax.fori_loop(0, SLOTS, normalise, 0, unroll=2)
    for cp in vector_out(0):
        cp.start()

    for n in range(NDEV - 1):
        pair_landed(n)
    for cp in own:
        cp.wait()
    spread = (lax.div(lax.broadcasted_iota(jnp.int32, (256, 16), 0), 16)
              == lax.broadcasted_iota(jnp.int32, (256, 16), 1)).astype(jnp.float32).astype(jnp.bfloat16)
    same = (lax.rem(lax.broadcasted_iota(jnp.int32, (256, 256), 0), 16)
            == lax.rem(lax.broadcasted_iota(jnp.int32, (256, 256), 1), 16))

    def piece(n):
        vbuf[lax.div(n, NP), lax.rem(n, NP)] = (
            sig[:, lanes(lax.rem(n, SLOTS))] * scale[0:1, :]).astype(jnp.bfloat16)

    def opening_pieces(k, carry):
        tall = jnp.dot(spread, wall[k], preferred_element_type=jnp.float32).astype(jnp.bfloat16)
        full = lax.dot_general(tall, spread, (((1,), (1,)), ((), ())), preferred_element_type=jnp.float32)
        kron[k] = jnp.where(same, full, 0.0).astype(jnp.bfloat16)
        for t in range(4):
            n = 4 * k + t
            psi_copy(n).wait()
            piece(n)
            psi_copy(n + SLOTS).start()
        return carry

    with jax.named_scope('convert'):
        lax.fori_loop(0, TERMS, opening_pieces, 0)
    left_landed(0)
    regroup(me)
    first_half = lax.rem(lax.broadcasted_iota(jnp.int32, (256, 256), 0), 16) < 8

    def mix(n, carry):
        kmix[n] = jnp.where(first_half, kron[2 * n].astype(jnp.float32),
                            kron[2 * n + 1].astype(jnp.float32)).astype(jnp.bfloat16)
        return carry

    lax.fori_loop(0, TERMS // 2, mix, 0)
    with jax.named_scope('ownwait'):
        for cp in place_own:
            cp.wait()

    chip = lax.div(me, 2)

    def group(rel):
        return chip + lax.rem(rel, 2) * (1 - 2 * xpos) + lax.div(rel, 2) * (2 - 4 * ypos)

    def place(j, u):
        later = lax.div(j + STEPS - 1, STEPS)
        t = lax.div(u, NCH)
        mid, last = lax.div(t * (3 - t), 2), lax.div(t, 3)
        rel0 = mid * (1 + lax.rem(u + 1, 2)) + last * 3
        c0 = (1 - mid - last) * u + mid * lax.div(u - NCH, 2) + last * (u - 3 * NCH)
        c = later * lax.div(u, NKG) + (1 - later) * c0
        rel = later * lax.rem(u, NKG) + (1 - later) * rel0
        return c, rel, group(rel)

    def fetch_start(j, u, slot):
        c, _, kg = place(j, u)
        pltpu.make_async_copy(rall_h.at[pl.ds(kg * KG, KG), :, lanes(c)], rblk.at[slot], r_sem.at[slot]).start()

    def fetch_wait(slot):
        pltpu.make_async_copy(rall_h.at[pl.ds(0, KG), :, lanes(0)], rblk.at[slot], r_sem.at[slot]).wait()

    def stage_left(j, s, g):
        for i in range(NKG):
            c, _, kg = place(j, NKG * s + i)
            rhs = jnp.concatenate([vbuf[c, 4 * g + t] for t in range(4)], axis=1)
            lhs = left[pl.ds(kg * KG, KG)].reshape(KG * ROWS, BOND)
            o = jnp.dot(lhs, rhs, preferred_element_type=jnp.float32).astype(jnp.bfloat16)
            for t in range(4):
                ubuf[4 * g + t, i * KG * ROWS:(i + 1) * KG * ROWS, :] = o[:, t * LANES:(t + 1) * LANES]

    def stage_pair(j, s):
        for i in range(NKG):
            _, _, kg = place(j, NKG * s + i)

            def columns(row):
                return ubuf[:, row:row + 16, :].reshape(256, LANES)

            for k in range(KG):
                row, at = (i * KG + k) * ROWS, k * LANES
                rhs = jnp.concatenate([columns(row + g * 16) for g in range(TAIL // 16)], axis=1)
                o = jnp.dot(kron[kg * KG + k], rhs, preferred_element_type=jnp.float32).astype(jnp.bfloat16)
                for g in range(TAIL // 16):
                    for q in range(NP):
                        zbuf[i, q * ROWS + g * 16:q * ROWS + (g + 1) * 16, at:at + LANES] = (
                            o[q * 16:(q + 1) * 16, g * LANES:(g + 1) * LANES])
            for n in range(KG // 2):
                row = (i * KG + 2 * n) * ROWS + TAIL
                rhs = jnp.concatenate([columns(row), columns(row + ROWS)], axis=1)
                o = jnp.dot(kmix[kg * (KG // 2) + n], rhs, preferred_element_type=jnp.float32)
                for h in range(2):
                    at = (2 * n + h) * LANES
                    for q in range(NP):
                        half = o[q * 16 + 8 * h:q * 16 + 8 * h + 8]
                        zbuf[i, q * ROWS + TAIL:(q + 1) * ROWS, at:at + LANES] = jnp.concatenate(
                            [half[:, :LANES], half[:, LANES:]], axis=0).astype(jnp.bfloat16)

    def stage_right(blocks, part):
        n0, n1 = NS[part][0] * LANES, NS[part][1] * LANES
        lhs = jnp.concatenate([rblk[slot, k] for _, slot in blocks for k in range(KG)], axis=1)
        rhs = jnp.concatenate([zbuf[i, n0:n1, :] for i, _ in blocks], axis=1)
        sig[:, n0:n1] += lax.dot_general(lhs, rhs, (((1,), (1,)), ((), ())), preferred_element_type=jnp.float32)

    def one_step(j, carry):
        beta_prev, cross = carry

        def r_before(q):
            for at, group in ((NKG, (1, 2)), (2 * NKG, (3, 4)), (5 * NKG, (5, 6))):
                @pl.when(q == at)
                def _(group=group):
                    for n in group:
                        left_landed(n)

            @pl.when((q >= 8) & (q < 8 + 2 * NCH) & (lax.rem(q, 2) == 0))
            def _():
                c = lax.div(q - 8, 2)
                for kind in (0, 2, 1, 3):
                    r_landed(c, kind)
                for kind in (5, 6, 7, 8):
                    r_send(c, kind)

            @pl.when(q >= 22)
            def _():
                c = q - 22
                r_landed(c, 5)
                r_landed(c, 6)
                r_send(c, 9)

        def fetch(u, slot=None):
            @pl.when(j == 0)
            def _():
                @pl.when(u < NCH)
                def _():
                    r_landed(u, 4)

                for odd, kind in ((1, 7), (0, 8)):
                    @pl.when((u >= NCH) & (u < 3 * NCH) & (lax.rem(u, 2) == odd))
                    def _(kind=kind):
                        r_landed(lax.div(u - NCH, 2), kind)

                @pl.when(u >= 3 * NCH)
                def _():
                    r_landed(u - 3 * NCH, 9)

            fetch_start(j, u, lax.rem(u, NKG) if slot is None else slot)

        def opening(g, carry):
            with jax.named_scope('first'):
                near, own = g + 1, g + 3
                relay_xy(lax.div(near, NKG), lax.rem(near, NKG))
                send_own(lax.div(own, NKG), lax.rem(own, NKG))
                relay_diag(0, g)
                arrived(0, g)
            with jax.named_scope('L'):
                stage_left(j, 0, g)
            return carry

        def opening_zero(g, carry):
            each = 12
            for t in range(each):
                psi_copy(4 * NP + each * g + t).wait()
            for t in range(each):
                piece(4 * NP + each * g + t)
            for t in range(each):
                n = 4 * NP + each * g + t + SLOTS

                @pl.when(n < NP * NCH)
                def _():
                    psi_copy(n).start()
            stage_left(j, 0, g)
            return carry

        @pl.when(j == 0)
        def _():
            with jax.named_scope('L0'):
                lax.fori_loop(0, NKG, opening_zero, 0)
                sig[...] = jnp.zeros((BOND, SLAB), jnp.float32)

        @pl.when(j > 0)
        def _():
            relay_xy(0, 0)
            send_own(0, 2)
            lax.fori_loop(0, NKG, opening, 0)
            with jax.named_scope('first3'):
                relay_xy(1, 1)
                send_own(1, 3)
                relay_diag(1, 0)
        for u in range(3):
            fetch(u)
        with jax.named_scope('W'):
            stage_pair(j, 0)

        def chunk(s, carry):
            def unit(g, carry):
                with jax.named_scope('before'):
                    @pl.when(j == 0)
                    def _():
                        r_before(NKG * s + g)

                    @pl.when(j > 0)
                    def _():
                        relay_diag(s, g + 1)

                        @pl.when(NKG * s + g < UNITS - 2)
                        def _():
                            ahead = g + 2
                            relay_xy(s + lax.div(ahead, NKG), lax.rem(ahead, NKG))

                        @pl.when(s < NCH - 1)
                        def _():
                            send_own(s + 1, g)

                        arrived(s, g)
                with jax.named_scope('RL'):
                    fetch_wait(g)
                    stage_left(j, s, g)
                    for part in range(len(NS)):
                        stage_right(((g, g),), part)
                with jax.named_scope('after'):
                    fetch(NKG * s + g - 1)
                return carry

            lax.fori_loop(0, NKG - 1, unit, 0)
            with jax.named_scope('before'):
                @pl.when(j == 0)
                def _():
                    r_before(NKG * s + NKG - 1)

                @pl.when(j > 0)
                def _():
                    @pl.when(s < NCH - 1)
                    def _():
                        relay_diag(s + 1, 0)
                        relay_xy(s + 1, 1)
                        send_own(s + 1, 3)

                    @pl.when(s == NCH - 1)
                    def _():
                        fetch_start(j, UNITS - 2, NKG - 2)
                        fetch_start(j, UNITS - 1, NKG)

                    arrived(s, NKG - 1)
            with jax.named_scope('LRW'):
                fetch_wait(NKG - 1)
                stage_left(j, s, NKG - 1)
                for part in range(len(NS)):
                    stage_right(((NKG - 1, NKG - 1),), part)
                stage_pair(j, s)
            with jax.named_scope('after'):
                @pl.when((j == 0) | (s < NCH - 1))
                def _():
                    fetch(NKG * s + 2)
            return carry

        lax.fori_loop(1, NCH, chunk, 0)

        @pl.when(j == 0)
        def _():
            r_before(UNITS)
            fetch(UNITS - 1, NKG)

        with jax.named_scope('sent'):
            @pl.when(j == 0)
            def _():
                for kind in range(NR):
                    r_sent(kind)
                for n in range(NDEV - 1):
                    for h in range(2):
                        left_copy(n, h).wait_send()
                    pair_copy(n).wait_send()

            @pl.when(j > 0)
            def _():
                for kind in range(len(v_kinds)):
                    v_sent(kind)

        with jax.named_scope('tail'):
            blocks = ((0, 0), (1, 1), (2, 2), (3, NKG))
            for _, slot in blocks:
                fetch_wait(slot)
            b_sum, v_sum = zero, zero
            for part in range(len(NS)):
                stage_right(blocks, part)
                for i in range(*NS[part]):
                    at = slice(i * LANES, (i + 1) * LANES)
                    for c in range(NCH):
                        cs = slice(c * LANES, (c + 1) * LANES)
                        s = sig[cs, at].T
                        v = vec[at, cs]
                        sig[cs, at] = s
                        b_sum = b_sum + fold(s * v)
                        v_sum = v_sum + fold(v * v)

        b_row = jnp.full((8, LANES), jnp.sum(b_sum))
        v_row = jnp.full((8, LANES), jnp.sum(v_sum))
        a_row = b_row + beta_prev * cross
        fit = jnp.where(v_row > 0, b_row / jnp.where(v_row > 0, v_row, 1.0), 0.0)
        fit_row = fit[0:1, :]

        def second(i, n_sum):
            at = pl.ds(pl.multiple_of(i * LANES, LANES), LANES)
            for c in range(NCH):
                cs = slice(c * LANES, (c + 1) * LANES)
                d = sig[cs, at] - fit_row * vec[at, cs]
                n_sum = n_sum + fold(d * d)
            return n_sum

        with jax.named_scope('pass2'):
            n_loc = jnp.sum(lax.fori_loop(0, SLOTS, second, zero, unroll=2))
        for cp in vector_out(j):
            cp.wait()

        row_id = lax.broadcasted_iota(jnp.int32, (8, LANES), 0)
        mine[...] = jnp.where(row_id == 0, a_row, jnp.where(
            row_id == 1, v_row, jnp.where(row_id == 2, fit, jnp.full((8, LANES), n_loc))))
        par = lax.rem(j, 2)
        with jax.named_scope('exch'):
            exchange_wait(par, exchange_start(par))
        total = exch[par, 0]
        for d in range(1, NDEV):
            total = total + exch[par, d]
        alpha = total[0:1, :] * (1.0 / ELEMS)
        square = jnp.zeros((1, LANES), jnp.float32)
        for d in range(NDEV):
            part = exch[par, d]
            gap = alpha - part[2:3, :]
            square = square + (part[3:4, :] + gap * gap * part[1:2, :])
        beta = jnp.sqrt(square * (1.0 / ELEMS))
        inv = 1.0 / beta
        ab_ref[j] = jnp.concatenate([alpha, beta] + [alpha] * 6, axis=0)

        def third(c, x_sum):
            cs = lanes(c)
            for i in range(SLOTS):
                at = slice(i * LANES, (i + 1) * LANES)
                v = vec[at, cs]
                n = (sig[cs, at] - alpha * v) * inv
                x_sum = x_sum + fold(v * n)
                vec[at, cs] = n
                low = n.astype(jnp.bfloat16)
                for t in range(8):
                    p, a = divmod(8 * i + t, ROWS // 16)
                    vbuf[c, p, pl.ds(pl.multiple_of(me * ROWS + 16 * a, 16), 16), :] = low[16 * t:16 * t + 16]
                sig[cs, at] = (v * -beta).T

            @pl.when((c < 2) & (j < STEPS - 1))
            def _():
                send_own(0, c)

            chunk_out(j + 1, c)
            return x_sum

        with jax.named_scope('pass3'):
            x_sum = lax.fori_loop(0, NCH, third, zero)
        return beta, jnp.full((8, LANES), jnp.sum(x_sum))

    lax.fori_loop(0, STEPS, one_step, (jnp.zeros((1, LANES), jnp.float32), zero))
    for cp in vector_out(STEPS):
        cp.wait()


def lanczos(psi, left, pair, right):
    dma = pltpu.SemaphoreType.DMA
    return pl.pallas_call(
        kernel,
        out_shape=(jax.ShapeDtypeStruct((STEPS + 1, ROWS, 4, 4, BOND), jnp.float32),
                   jax.ShapeDtypeStruct((TERMS, BOND, BOND), jnp.bfloat16),
                   jax.ShapeDtypeStruct((STEPS, 8, LANES), jnp.float32)),
        in_specs=[pl.BlockSpec(memory_space=pl.ANY)] * 4,
        out_specs=(pl.BlockSpec(memory_space=pl.ANY), pl.BlockSpec(memory_space=pl.ANY),
                   pl.BlockSpec(memory_space=pltpu.VMEM)),
        scratch_shapes=[
            pltpu.VMEM((NCH, NP, BOND, LANES), jnp.bfloat16),
            pltpu.VMEM((TERMS, ROWS, BOND), jnp.bfloat16),
            pltpu.VMEM((TERMS, 16, 16), jnp.bfloat16),
            pltpu.VMEM((TERMS, 256, 256), jnp.bfloat16),
            pltpu.VMEM((TERMS // 2, 256, 256), jnp.bfloat16),
            pltpu.VMEM((NKG + 1, KG, BOND, LANES), jnp.bfloat16),
            pltpu.VMEM((BOND, SLAB), jnp.float32),
            pltpu.VMEM((NP, TERMS * ROWS, LANES), jnp.bfloat16),
            pltpu.VMEM((NKG, SLAB, KG * LANES), jnp.bfloat16),
            pltpu.VMEM((SLAB, BOND), jnp.float32),
            pltpu.VMEM((8, LANES), jnp.float32),
            pltpu.VMEM((8, LANES), jnp.float32),
            pltpu.VMEM((2, NDEV, 8, LANES), jnp.float32),
            dma((NP,)), dma((SLOTS,)), dma((2,)), dma((2 * NCH,)), dma((14,)), dma((14,)), dma((NDEV - 1,)), dma((NDEV - 1,)),
            dma((NKG + 1,)), dma((NP,)), dma((10,)), dma((UNITS * 4,)), dma((NDEV - 1,)), dma((2, NDEV - 1)),
        ],
        compiler_params=pltpu.CompilerParams(collective_id=0, has_side_effects=True, vmem_limit_bytes=67043328),
    )(psi, left, pair, right)


def solution(mesh):
    def local_run(psi_init, left_env, op_pair, right_env):
        vectors, _, ab = lanczos(psi_init, left_env, op_pair, right_env)
        return vectors, ab[:, 0, 0], ab[:, 1, 0]

    return jax.shard_map(local_run, mesh=mesh, in_specs=(P(), P('terms'), P('terms'), P('terms')),
                         out_specs=(P(None, 'terms'), P(), P()), check_vma=False)
```

```python
import jax
import jax.numpy as jnp
from jax import lax
from jax.experimental import pallas as pl
from jax.experimental.pallas import tpu as pltpu
from jax.sharding import PartitionSpec as P

STEPS = 6
BOND = 896
NP = 16
TERMS = 16
NDEV = 8
ROWS = BOND // NDEV
LANES = 128
NCH = BOND // LANES
KG = 4
NKG = TERMS // KG
UNITS = NCH * NKG
SLAB = NP * ROWS
SLOTS = SLAB // LANES
TAIL = 96
ELEMS = BOND * NP * BOND
MESH = pl.DeviceIdType.MESH
NS = ((0, 4), (4, 8), (8, 12), (12, 14))


def kernel(psi_h, left_h, pair_h, right_h, kry_h, rall_h, ab_ref,
           vbuf, left, wall, kron, kmix, rblk, sig, ubuf, zbuf, vec, scale, mine, exch,
           slab_sem, psi_sem, own_sem, rest_sem, ls_sem, lr_sem, ws_sem, wr_sem,
           r_sem, out_sem, send_sem, recv_sem, xs_sem, xr_sem):
    me = lax.axis_index('terms')
    core = lax.rem(me, 2)
    xpos = lax.rem(lax.div(me, 2), 2)
    ypos = lax.div(me, 4)
    sib = me + 1 - 2 * core
    xn = me + 2 - 4 * xpos
    yn = me + 4 - 8 * ypos
    dg = yn + 2 - 4 * xpos
    sx = xn + 1 - 2 * core
    sy = yn + 1 - 2 * core
    sd = dg + 1 - 2 * core
    others = (sib, xn, sx, yn, sy, dg, sd)

    def rows(dev):
        return pl.ds(pl.multiple_of(dev * ROWS, 16), ROWS)

    def lanes(c):
        return pl.ds(pl.multiple_of(c * LANES, LANES), LANES)

    def remote(src, dst, ssem, rsem, target):
        return pltpu.make_async_remote_copy(src, dst, ssem, rsem, device_id=(target,), device_id_type=MESH)

    v_kinds = ((0, 4, me, xn, 0), (0, 4, me, yn, 1), (0, 4, me, sib, 3), (0, 2, xn, yn, 2), (2, 2, yn, xn, 2),
               (0, 4, xn, sib, 3), (0, 4, yn, sib, 3), (0, 4, dg, sib, 3))
    v_arrivals = (4, 4, 4, 16)
    NV = len(v_arrivals)

    def v_part(first, count, origin, c, g):
        return vbuf.at[c, pl.ds(4 * g + first, count), rows(origin), :]

    def v_sem(c, g, arrival):
        return recv_sem.at[c * (NV * NKG) + g * NV + arrival]

    def v_send(c, g, kind):
        first, count, origin, target, arrival = v_kinds[kind]
        part = v_part(first, count, origin, c, g)
        remote(part, part, send_sem.at[kind], v_sem(c, g, arrival), target).start()

    def v_landed(c, g, arrival):
        part = vbuf.at[c, pl.ds(0, v_arrivals[arrival]), rows(me), :]
        remote(part, part, send_sem.at[0], v_sem(c, g, arrival), sib).wait_recv()

    def v_sent(kind):
        first, count, origin, target, _ = v_kinds[kind]
        part = vbuf.at[:, pl.ds(0, 4 * count), rows(origin), :]
        remote(part, part, send_sem.at[kind], recv_sem.at[kind], target).wait_send()

    def send_own(c, g):
        for kind in (0, 1, 2):
            v_send(c, g, kind)

    def relay_xy(c, g):
        v_landed(c, g, 0)
        v_send(c, g, 3)
        v_send(c, g, 5)
        v_landed(c, g, 1)
        v_send(c, g, 4)
        v_send(c, g, 6)

    def relay_diag(c, g):
        v_landed(c, g, 2)
        v_send(c, g, 7)

    def arrived(c, g):
        v_landed(c, g, 3)

    LO, HI, ALL = (0, 1), (1, 1), (0, 2)
    r_kinds = ((LO, me, xn, xn), (HI, me, xn, xn), (HI, me, yn, yn), (LO, me, yn, yn), (ALL, me, sib, sib),
               (LO, xn, yn, dg), (HI, yn, xn, dg), (ALL, xn, sib, sx), (ALL, yn, sib, sy), (ALL, dg, sib, sd))
    NR = len(r_kinds)

    def r_part(half, origin, c):
        return rall_h.at[pl.ds(2 * origin + half[0], half[1]), :, lanes(c)]

    def r_send(c, kind):
        half, origin, target, _ = r_kinds[kind]
        dst = r_part(half, origin, c)
        src = right_h.at[pl.ds(half[0], half[1]), :, lanes(c)] if kind < 5 else dst
        remote(src, dst, send_sem.at[kind], recv_sem.at[c * NR + kind], target).start()

    def r_landed(c, kind):
        half, _, target, origin = r_kinds[kind]
        part = r_part(half, origin, c)
        remote(part, part, send_sem.at[kind], recv_sem.at[c * NR + kind], target).wait_recv()

    def r_sent(kind):
        half, origin, target, _ = r_kinds[kind]
        part = rall_h.at[pl.ds(2 * origin + half[0], half[1])]
        remote(part, part, send_sem.at[kind], recv_sem.at[kind], target).wait_send()

    def left_copy(n, h):
        return remote(left_h.at[h, rows(others[n]), :], left.at[2 * me + h], ls_sem.at[2 * n + h], lr_sem.at[2 * n + h],
                      others[n])

    def regroup(dev):
        a, b = (left[2 * dev + h, TAIL:ROWS, :].astype(jnp.float32) for h in range(2))
        left[2 * dev, TAIL:ROWS, :] = jnp.concatenate([a[:8], b[:8]], axis=0).astype(jnp.bfloat16)
        left[2 * dev + 1, TAIL:ROWS, :] = jnp.concatenate([a[8:], b[8:]], axis=0).astype(jnp.bfloat16)

    def left_landed(n):
        for h in range(2):
            part = left.at[2 * others[n] + h]
            remote(part, part, ls_sem.at[2 * n + h], lr_sem.at[2 * n + h], others[n]).wait_recv()
        regroup(others[n])

    def pair_copy(n):
        return remote(pair_h, wall.at[pl.ds(2 * me, 2)], ws_sem.at[n], wr_sem.at[n], others[n])

    def pair_landed(n):
        part = wall.at[pl.ds(2 * others[n], 2)]
        remote(part, part, ws_sem.at[n], wr_sem.at[n], others[n]).wait_recv()

    def psi_copy(n):
        c, p, slot = lax.div(n, NP), lax.rem(n, NP), lax.rem(n, SLOTS)
        return pltpu.make_async_copy(psi_h.at[:, lax.div(p, 4), lax.rem(p, 4), lanes(c)], sig.at[:, lanes(slot)],
                                     psi_sem.at[slot])

    def vector_out(j):
        return [pltpu.make_async_copy(vec.at[pl.ds(p * ROWS, ROWS), :], kry_h.at[j, :, p // 4, p % 4, :],
                                      out_sem.at[p]) for p in range(NP)]

    def chunk_out(j, c):
        for p in range(NP):
            pltpu.make_async_copy(vec.at[pl.ds(p * ROWS, ROWS), lanes(c)], kry_h.at[j, :, p // 4, p % 4, lanes(c)],
                                  out_sem.at[p]).start()

    def fold(x):
        return jnp.sum(x.reshape(-1, 8, LANES), axis=0)

    def exchange_start(par):
        exch[par, me] = mine[...]
        copies = [remote(mine, exch.at[par, me], xs_sem.at[n], xr_sem.at[par, n], others[n]) for n in range(NDEV - 1)]
        for cp in copies:
            cp.start()
        return copies

    def exchange_wait(par, copies):
        for n in range(NDEV - 1):
            remote(mine, exch.at[par, others[n]], xs_sem.at[n], xr_sem.at[par, n], others[n]).wait_recv()
        for cp in copies:
            cp.wait_send()

    barrier = pltpu.get_barrier_semaphore()
    for n in range(NDEV - 1):
        pl.semaphore_signal(barrier, inc=1, device_id=(others[n],), device_id_type=MESH)
    slab = [pltpu.make_async_copy(psi_h.at[rows(me), p // 4, p % 4, :], vec.at[pl.ds(p * ROWS, ROWS), :],
                                  slab_sem.at[p]) for p in range(NP)]
    for cp in slab:
        cp.start()
    own = [pltpu.make_async_copy(pair_h, wall.at[pl.ds(2 * me, 2)], own_sem.at[0]),
           pltpu.make_async_copy(left_h.at[:, rows(me), :], left.at[pl.ds(2 * me, 2)], own_sem.at[1])]
    for cp in own:
        cp.start()
    rest = [(h, c, rblk.at[(h * NCH + c) // KG, (h * NCH + c) % KG]) for h in range(2) for c in range(NCH)]
    take = [pltpu.make_async_copy(right_h.at[h, :, lanes(c)], at, rest_sem.at[n]) for n, (h, c, at) in enumerate(rest)]
    place_own = [pltpu.make_async_copy(at, rall_h.at[2 * me + h, :, lanes(c)], rest_sem.at[n])
                 for n, (h, c, at) in enumerate(rest)]
    for cp in take:
        cp.start()
    for n in range(SLOTS):
        psi_copy(n).start()
    zero = jnp.zeros((8, LANES), jnp.float32)
    with jax.named_scope('barrier'):
        pl.semaphore_wait(barrier, NDEV - 1)
    for n, h in ((1, 0), (3, 0), (0, 0), (0, 1)):
        left_copy(n, h).start()
    for cp in slab:
        cp.wait()

    def squares(i, acc):
        at = pl.ds(pl.multiple_of(i * LANES, LANES), LANES)
        for c in range(NCH):
            x = vec[at, c * LANES:(c + 1) * LANES]
            acc = acc + fold(x * x)
        return acc

    mine[...] = jnp.full((8, LANES), jnp.sum(lax.fori_loop(0, SLOTS, squares, zero, unroll=2)))
    copies = exchange_start(1)
    for n in range(NDEV - 1):
        pair_copy(n).start()
    for n, h in ((1, 1), (3, 1), (2, 0), (4, 0), (2, 1), (4, 1)):
        left_copy(n, h).start()

    def r_own(c):
        for kind in (4, 0, 2, 1, 3):
            r_send(c, kind)

    def operators_out(c, carry):
        r_own(c)
        return carry

    lax.fori_loop(0, 5, operators_out, 0)
    for n in (5, 6):
        for h in range(2):
            left_copy(n, h).start()
    lax.fori_loop(5, NCH, operators_out, 0)
    for cp in take:
        cp.wait()
    for cp in place_own:
        cp.start()
    with jax.named_scope('exch0'):
        exchange_wait(1, copies)
    total = exch[1, 0]
    for d in range(1, NDEV):
        total = total + exch[1, d]
    scale[...] = 1.0 / jnp.sqrt(total * (1.0 / ELEMS))

    def normalise(i, carry):
        at = pl.ds(pl.multiple_of(i * LANES, LANES), LANES)
        for c in range(NCH):
            cs = slice(c * LANES, (c + 1) * LANES)
            vec[at, cs] = vec[at, cs] * scale[0:1, :]
        return carry

    lax.fori_loop(0, SLOTS, normalise, 0, unroll=2)
    for cp in vector_out(0):
        cp.start()

    for n in range(NDEV - 1):
        pair_landed(n)
    for cp in own:
        cp.wait()
    spread = (lax.div(lax.broadcasted_iota(jnp.int32, (256, 16), 0), 16)
              == lax.broadcasted_iota(jnp.int32, (256, 16), 1)).astype(jnp.float32).astype(jnp.bfloat16)
    same = (lax.rem(lax.broadcasted_iota(jnp.int32, (256, 256), 0), 16)
            == lax.rem(lax.broadcasted_iota(jnp.int32, (256, 256), 1), 16))

    def piece(n):
        vbuf[lax.div(n, NP), lax.rem(n, NP)] = (
            sig[:, lanes(lax.rem(n, SLOTS))] * scale[0:1, :]).astype(jnp.bfloat16)

    def opening_pieces(k, carry):
        tall = jnp.dot(spread, wall[k], preferred_element_type=jnp.float32).astype(jnp.bfloat16)
        full = lax.dot_general(tall, spread, (((1,), (1,)), ((), ())), preferred_element_type=jnp.float32)
        kron[k] = jnp.where(same, full, 0.0).astype(jnp.bfloat16)
        for t in range(4):
            n = 4 * k + t
            psi_copy(n).wait()
            piece(n)
            psi_copy(n + SLOTS).start()
        return carry

    with jax.named_scope('convert'):
        lax.fori_loop(0, TERMS, opening_pieces, 0)
    left_landed(0)
    regroup(me)
    first_half = lax.rem(lax.broadcasted_iota(jnp.int32, (256, 256), 0), 16) < 8

    def mix(n, carry):
        kmix[n] = jnp.where(first_half, kron[2 * n].astype(jnp.float32),
                            kron[2 * n + 1].astype(jnp.float32)).astype(jnp.bfloat16)
        return carry

    lax.fori_loop(0, TERMS // 2, mix, 0)
    with jax.named_scope('ownwait'):
        for cp in place_own:
            cp.wait()

    chip = lax.div(me, 2)

    def group(rel):
        return chip + lax.rem(rel, 2) * (1 - 2 * xpos) + lax.div(rel, 2) * (2 - 4 * ypos)

    def place(j, u):
        later = lax.div(j + STEPS - 1, STEPS)
        t = lax.div(u, NCH)
        mid, last = lax.div(t * (3 - t), 2), lax.div(t, 3)
        rel0 = mid * (1 + lax.rem(u + 1, 2)) + last * 3
        c0 = (1 - mid - last) * u + mid * lax.div(u - NCH, 2) + last * (u - 3 * NCH)
        c = later * lax.div(u, NKG) + (1 - later) * c0
        rel = later * lax.rem(u, NKG) + (1 - later) * rel0
        return c, rel, group(rel)

    def fetch_start(j, u, slot):
        c, _, kg = place(j, u)
        pltpu.make_async_copy(rall_h.at[pl.ds(kg * KG, KG), :, lanes(c)], rblk.at[slot], r_sem.at[slot]).start()

    def fetch_wait(slot):
        pltpu.make_async_copy(rall_h.at[pl.ds(0, KG), :, lanes(0)], rblk.at[slot], r_sem.at[slot]).wait()

    def stage_left(j, s, g):
        for i in range(NKG):
            c, _, kg = place(j, NKG * s + i)
            rhs = jnp.concatenate([vbuf[c, 4 * g + t] for t in range(4)], axis=1)
            lhs = left[pl.ds(kg * KG, KG)].reshape(KG * ROWS, BOND)
            o = jnp.dot(lhs, rhs, preferred_element_type=jnp.float32).astype(jnp.bfloat16)
            for t in range(4):
                ubuf[4 * g + t, i * KG * ROWS:(i + 1) * KG * ROWS, :] = o[:, t * LANES:(t + 1) * LANES]

    def stage_pair(j, s):
        for i in range(NKG):
            _, _, kg = place(j, NKG * s + i)

            def columns(row):
                return ubuf[:, row:row + 16, :].reshape(256, LANES)

            for k in range(KG):
                row, at = (i * KG + k) * ROWS, k * LANES
                rhs = jnp.concatenate([columns(row + g * 16) for g in range(TAIL // 16)], axis=1)
                o = jnp.dot(kron[kg * KG + k], rhs, preferred_element_type=jnp.float32).astype(jnp.bfloat16)
                for g in range(TAIL // 16):
                    for q in range(NP):
                        zbuf[i, q * ROWS + g * 16:q * ROWS + (g + 1) * 16, at:at + LANES] = (
                            o[q * 16:(q + 1) * 16, g * LANES:(g + 1) * LANES])
            for n in range(KG // 2):
                row = (i * KG + 2 * n) * ROWS + TAIL
                rhs = jnp.concatenate([columns(row), columns(row + ROWS)], axis=1)
                o = jnp.dot(kmix[kg * (KG // 2) + n], rhs, preferred_element_type=jnp.float32)
                for h in range(2):
                    at = (2 * n + h) * LANES
                    for q in range(NP):
                        half = o[q * 16 + 8 * h:q * 16 + 8 * h + 8]
                        zbuf[i, q * ROWS + TAIL:(q + 1) * ROWS, at:at + LANES] = jnp.concatenate(
                            [half[:, :LANES], half[:, LANES:]], axis=0).astype(jnp.bfloat16)

    def stage_right(blocks, part):
        n0, n1 = NS[part][0] * LANES, NS[part][1] * LANES
        lhs = jnp.concatenate([rblk[slot, k] for _, slot in blocks for k in range(KG)], axis=1)
        rhs = jnp.concatenate([zbuf[i, n0:n1, :] for i, _ in blocks], axis=1)
        sig[:, n0:n1] += lax.dot_general(lhs, rhs, (((1,), (1,)), ((), ())), preferred_element_type=jnp.float32)

    def one_step(j, carry):
        beta_prev, cross = carry

        def r_before(q):
            for at, group in ((NKG, (1, 2)), (2 * NKG, (3, 4)), (5 * NKG, (5, 6))):
                @pl.when(q == at)
                def _(group=group):
                    for n in group:
                        left_landed(n)

            @pl.when((q >= 8) & (q < 8 + 2 * NCH) & (lax.rem(q, 2) == 0))
            def _():
                c = lax.div(q - 8, 2)
                for kind in (0, 2, 1, 3):
                    r_landed(c, kind)
                for kind in (5, 6, 7, 8):
                    r_send(c, kind)

            @pl.when(q >= 22)
            def _():
                c = q - 22
                r_landed(c, 5)
                r_landed(c, 6)
                r_send(c, 9)

        def fetch(u, slot=None):
            @pl.when(j == 0)
            def _():
                @pl.when(u < NCH)
                def _():
                    r_landed(u, 4)

                for odd, kind in ((1, 7), (0, 8)):
                    @pl.when((u >= NCH) & (u < 3 * NCH) & (lax.rem(u, 2) == odd))
                    def _(kind=kind):
                        r_landed(lax.div(u - NCH, 2), kind)

                @pl.when(u >= 3 * NCH)
                def _():
                    r_landed(u - 3 * NCH, 9)

            fetch_start(j, u, lax.rem(u, NKG) if slot is None else slot)

        def opening(g, carry):
            with jax.named_scope('first'):
                near, own = g + 1, g + 3
                relay_xy(lax.div(near, NKG), lax.rem(near, NKG))
                send_own(lax.div(own, NKG), lax.rem(own, NKG))
                relay_diag(0, g)
                arrived(0, g)
            with jax.named_scope('L'):
                stage_left(j, 0, g)
            return carry

        def opening_zero(g, carry):
            each = 12
            for t in range(each):
                psi_copy(4 * NP + each * g + t).wait()
            for t in range(each):
                piece(4 * NP + each * g + t)
            for t in range(each):
                n = 4 * NP + each * g + t + SLOTS

                @pl.when(n < NP * NCH)
                def _():
                    psi_copy(n).start()
            stage_left(j, 0, g)
            return carry

        @pl.when(j == 0)
        def _():
            with jax.named_scope('L0'):
                lax.fori_loop(0, NKG, opening_zero, 0)
                sig[...] = jnp.zeros((BOND, SLAB), jnp.float32)

        @pl.when(j > 0)
        def _():
            relay_xy(0, 0)
            send_own(0, 2)
            lax.fori_loop(0, NKG, opening, 0)
            with jax.named_scope('first3'):
                relay_xy(1, 1)
                send_own(1, 3)
                relay_diag(1, 0)
        for u in range(3):
            fetch(u)
        with jax.named_scope('W'):
            stage_pair(j, 0)

        def chunk(s, carry):
            def unit(g, carry):
                with jax.named_scope('before'):
                    @pl.when(j == 0)
                    def _():
                        r_before(NKG * s + g)

                    @pl.when(j > 0)
                    def _():
                        @pl.when(NKG * s + g < UNITS - 2)
                        def _():
                            ahead = g + 2
                            relay_xy(s + lax.div(ahead, NKG), lax.rem(ahead, NKG))

                        @pl.when(s < NCH - 1)
                        def _():
                            send_own(s + 1, g)

                        relay_diag(s, g + 1)
                        arrived(s, g)
                with jax.named_scope('RL'):
                    fetch_wait(g)
                    stage_left(j, s, g)
                    for part in range(len(NS)):
                        stage_right(((g, g),), part)
                with jax.named_scope('after'):
                    fetch(NKG * s + g - 1)
                return carry

            lax.fori_loop(0, NKG - 1, unit, 0)
            with jax.named_scope('before'):
                @pl.when(j == 0)
                def _():
                    r_before(NKG * s + NKG - 1)

                @pl.when(j > 0)
                def _():
                    @pl.when(s < NCH - 1)
                    def _():
                        relay_diag(s + 1, 0)
                        relay_xy(s + 1, 1)
                        send_own(s + 1, 3)

                    @pl.when(s == NCH - 1)
                    def _():
                        fetch_start(j, UNITS - 2, NKG - 2)
                        fetch_start(j, UNITS - 1, NKG)

                    arrived(s, NKG - 1)
            with jax.named_scope('LRW'):
                fetch_wait(NKG - 1)
                stage_left(j, s, NKG - 1)
                for part in range(len(NS)):
                    stage_right(((NKG - 1, NKG - 1),), part)
                stage_pair(j, s)
            with jax.named_scope('after'):
                @pl.when((j == 0) | (s < NCH - 1))
                def _():
                    fetch(NKG * s + 2)
            return carry

        lax.fori_loop(1, NCH, chunk, 0)

        @pl.when(j == 0)
        def _():
            r_before(UNITS)
            fetch(UNITS - 1, NKG)

        with jax.named_scope('sent'):
            @pl.when(j == 0)
            def _():
                for kind in range(NR):
                    r_sent(kind)
                for n in range(NDEV - 1):
                    for h in range(2):
                        left_copy(n, h).wait_send()
                    pair_copy(n).wait_send()

            @pl.when(j > 0)
            def _():
                for kind in range(len(v_kinds)):
                    v_sent(kind)

        with jax.named_scope('tail'):
            blocks = ((0, 0), (1, 1), (2, 2), (3, NKG))
            for _, slot in blocks:
                fetch_wait(slot)
            b_sum, v_sum = zero, zero
            for part in range(len(NS)):
                stage_right(blocks, part)
                for i in range(*NS[part]):
                    at = slice(i * LANES, (i + 1) * LANES)
                    for c in range(NCH):
                        cs = slice(c * LANES, (c + 1) * LANES)
                        s = sig[cs, at].T
                        v = vec[at, cs]
                        sig[cs, at] = s
                        b_sum = b_sum + fold(s * v)
                        v_sum = v_sum + fold(v * v)

        b_row = jnp.full((8, LANES), jnp.sum(b_sum))
        v_row = jnp.full((8, LANES), jnp.sum(v_sum))
        a_row = b_row + beta_prev * cross
        held = v_row > 1e-20
        fit = jnp.where(held, b_row / jnp.where(held, v_row, 1.0), 0.0)
        fit_row = fit[0:1, :]

        def second(i, n_sum):
            at = pl.ds(pl.multiple_of(i * LANES, LANES), LANES)
            for c in range(NCH):
                cs = slice(c * LANES, (c + 1) * LANES)
                d = sig[cs, at] - fit_row * vec[at, cs]
                n_sum = n_sum + fold(d * d)
            return n_sum

        with jax.named_scope('pass2'):
            n_loc = jnp.sum(lax.fori_loop(0, SLOTS, second, zero, unroll=2))
        for cp in vector_out(j):
            cp.wait()

        row_id = lax.broadcasted_iota(jnp.int32, (8, LANES), 0)
        mine[...] = jnp.where(row_id == 0, a_row, jnp.where(
            row_id == 1, jnp.sqrt(v_row), jnp.where(row_id == 2, fit, jnp.full((8, LANES), n_loc))))
        par = lax.rem(j, 2)
        with jax.named_scope('exch'):
            exchange_wait(par, exchange_start(par))
        total = exch[par, 0]
        for d in range(1, NDEV):
            total = total + exch[par, d]
        alpha = total[0:1, :] * (1.0 / ELEMS)
        square = jnp.zeros((1, LANES), jnp.float32)
        for d in range(NDEV):
            part = exch[par, d]
            gap = (alpha - part[2:3, :]) * part[1:2, :]
            square = square + (part[3:4, :] + gap * gap)
        beta = jnp.sqrt(square * (1.0 / ELEMS))
        inv = 1.0 / beta
        ab_ref[j] = jnp.concatenate([alpha, beta] + [alpha] * 6, axis=0)

        def third(c, x_sum):
            cs = lanes(c)
            for i in range(SLOTS):
                at = slice(i * LANES, (i + 1) * LANES)
                v = vec[at, cs]
                n = (sig[cs, at] - alpha * v) * inv
                x_sum = x_sum + fold(v * n)
                vec[at, cs] = n
                low = n.astype(jnp.bfloat16)
                for t in range(8):
                    p, a = divmod(8 * i + t, ROWS // 16)
                    vbuf[c, p, pl.ds(pl.multiple_of(me * ROWS + 16 * a, 16), 16), :] = low[16 * t:16 * t + 16]
                sig[cs, at] = (v * -beta).T

            @pl.when((c < 2) & (j < STEPS - 1))
            def _():
                send_own(0, c)

            chunk_out(j + 1, c)
            return x_sum

        with jax.named_scope('pass3'):
            x_sum = lax.fori_loop(0, NCH, third, zero)
        return beta, jnp.full((8, LANES), jnp.sum(x_sum))

    lax.fori_loop(0, STEPS, one_step, (jnp.zeros((1, LANES), jnp.float32), zero))
    for cp in vector_out(STEPS):
        cp.wait()


def lanczos(psi, left, pair, right):
    dma = pltpu.SemaphoreType.DMA
    return pl.pallas_call(
        kernel,
        out_shape=(jax.ShapeDtypeStruct((STEPS + 1, ROWS, 4, 4, BOND), jnp.float32),
                   jax.ShapeDtypeStruct((TERMS, BOND, BOND), jnp.bfloat16),
                   jax.ShapeDtypeStruct((STEPS, 8, LANES), jnp.float32)),
        in_specs=[pl.BlockSpec(memory_space=pl.ANY)] * 4,
        out_specs=(pl.BlockSpec(memory_space=pl.ANY), pl.BlockSpec(memory_space=pl.ANY),
                   pl.BlockSpec(memory_space=pltpu.VMEM)),
        scratch_shapes=[
            pltpu.VMEM((NCH, NP, BOND, LANES), jnp.bfloat16),
            pltpu.VMEM((TERMS, ROWS, BOND), jnp.bfloat16),
            pltpu.VMEM((TERMS, 16, 16), jnp.bfloat16),
            pltpu.VMEM((TERMS, 256, 256), jnp.bfloat16),
            pltpu.VMEM((TERMS // 2, 256, 256), jnp.bfloat16),
            pltpu.VMEM((NKG + 1, KG, BOND, LANES), jnp.bfloat16),
            pltpu.VMEM((BOND, SLAB), jnp.float32),
            pltpu.VMEM((NP, TERMS * ROWS, LANES), jnp.bfloat16),
            pltpu.VMEM((NKG, SLAB, KG * LANES), jnp.bfloat16),
            pltpu.VMEM((SLAB, BOND), jnp.float32),
            pltpu.VMEM((8, LANES), jnp.float32),
            pltpu.VMEM((8, LANES), jnp.float32),
            pltpu.VMEM((2, NDEV, 8, LANES), jnp.float32),
            dma((NP,)), dma((SLOTS,)), dma((2,)), dma((2 * NCH,)), dma((14,)), dma((14,)), dma((NDEV - 1,)), dma((NDEV - 1,)),
            dma((NKG + 1,)), dma((NP,)), dma((10,)), dma((UNITS * 4,)), dma((NDEV - 1,)), dma((2, NDEV - 1)),
        ],
        compiler_params=pltpu.CompilerParams(collective_id=0, has_side_effects=True, vmem_limit_bytes=67043328),
    )(psi, left, pair, right)


def solution(mesh):
    def local_run(psi_init, left_env, op_pair, right_env):
        vectors, _, ab = lanczos(psi_init, left_env, op_pair, right_env)
        return vectors, ab[:, 0, 0], ab[:, 1, 0]

    return jax.shard_map(local_run, mesh=mesh, in_specs=(P(), P('terms'), P('terms'), P('terms')),
                         out_specs=(P(None, 'terms'), P(), P()), check_vma=False)
```

```python
import jax
import jax.numpy as jnp
from jax import lax
from jax.experimental import pallas as pl
from jax.experimental.pallas import tpu as pltpu
from jax.sharding import PartitionSpec as P

STEPS = 6
BOND = 896
NP = 16
TERMS = 16
NDEV = 8
ROWS = BOND // NDEV
LANES = 128
NCH = BOND // LANES
KG = 4
NKG = TERMS // KG
UNITS = NCH * NKG
SLAB = NP * ROWS
SLOTS = SLAB // LANES
TAIL = 96
ELEMS = BOND * NP * BOND
MESH = pl.DeviceIdType.MESH
NS = ((0, 4), (4, 8), (8, 12), (12, 14))


def kernel(psi_h, left_h, pair_h, right_h, kry_h, rall_h, ab_ref,
           vbuf, left, wall, kron, kmix, rblk, sig, ubuf, zbuf, vec, scale, mine, exch,
           slab_sem, psi_sem, own_sem, rest_sem, ls_sem, lr_sem, ws_sem, wr_sem,
           r_sem, out_sem, send_sem, recv_sem, xs_sem, xr_sem):
    me = lax.axis_index('terms')
    core = lax.rem(me, 2)
    xpos = lax.rem(lax.div(me, 2), 2)
    ypos = lax.div(me, 4)
    sib = me + 1 - 2 * core
    xn = me + 2 - 4 * xpos
    yn = me + 4 - 8 * ypos
    dg = yn + 2 - 4 * xpos
    sx = xn + 1 - 2 * core
    sy = yn + 1 - 2 * core
    sd = dg + 1 - 2 * core
    others = (sib, xn, sx, yn, sy, dg, sd)

    def rows(dev):
        return pl.ds(pl.multiple_of(dev * ROWS, 16), ROWS)

    def lanes(c):
        return pl.ds(pl.multiple_of(c * LANES, LANES), LANES)

    def remote(src, dst, ssem, rsem, target):
        return pltpu.make_async_remote_copy(src, dst, ssem, rsem, device_id=(target,), device_id_type=MESH)

    v_kinds = ((0, 4, me, xn, 0), (0, 4, me, yn, 1), (0, 4, me, sib, 3), (0, 2, xn, yn, 2), (2, 2, yn, xn, 2),
               (0, 4, xn, sib, 3), (0, 4, yn, sib, 3), (0, 4, dg, sib, 3))
    v_arrivals = (4, 4, 4, 16)
    NV = len(v_arrivals)

    def v_part(first, count, origin, c, g):
        return vbuf.at[c, pl.ds(4 * g + first, count), rows(origin), :]

    def v_sem(c, g, arrival):
        return recv_sem.at[c * (NV * NKG) + g * NV + arrival]

    def v_send(c, g, kind):
        first, count, origin, target, arrival = v_kinds[kind]
        part = v_part(first, count, origin, c, g)
        remote(part, part, send_sem.at[kind], v_sem(c, g, arrival), target).start()

    def v_landed(c, g, arrival):
        part = vbuf.at[c, pl.ds(0, v_arrivals[arrival]), rows(me), :]
        remote(part, part, send_sem.at[0], v_sem(c, g, arrival), sib).wait_recv()

    def v_sent(kind):
        first, count, origin, target, _ = v_kinds[kind]
        part = vbuf.at[:, pl.ds(0, 4 * count), rows(origin), :]
        remote(part, part, send_sem.at[kind], recv_sem.at[kind], target).wait_send()

    def send_own(c, g):
        for kind in (0, 1, 2):
            v_send(c, g, kind)

    def relay_xy(c, g):
        v_landed(c, g, 0)
        v_send(c, g, 3)
        v_send(c, g, 5)
        v_landed(c, g, 1)
        v_send(c, g, 4)
        v_send(c, g, 6)

    def relay_diag(c, g):
        v_landed(c, g, 2)
        v_send(c, g, 7)

    def arrived(c, g):
        v_landed(c, g, 3)

    LO, HI, ALL = (0, 1), (1, 1), (0, 2)
    r_kinds = ((LO, me, xn, xn), (HI, me, xn, xn), (HI, me, yn, yn), (LO, me, yn, yn), (ALL, me, sib, sib),
               (LO, xn, yn, dg), (HI, yn, xn, dg), (ALL, xn, sib, sx), (ALL, yn, sib, sy), (ALL, dg, sib, sd))
    NR = len(r_kinds)

    def r_part(half, origin, c):
        return rall_h.at[pl.ds(2 * origin + half[0], half[1]), :, lanes(c)]

    def r_send(c, kind):
        half, origin, target, _ = r_kinds[kind]
        dst = r_part(half, origin, c)
        src = right_h.at[pl.ds(half[0], half[1]), :, lanes(c)] if kind < 5 else dst
        remote(src, dst, send_sem.at[kind], recv_sem.at[c * NR + kind], target).start()

    def r_landed(c, kind):
        half, _, target, origin = r_kinds[kind]
        part = r_part(half, origin, c)
        remote(part, part, send_sem.at[kind], recv_sem.at[c * NR + kind], target).wait_recv()

    def r_sent(kind):
        half, origin, target, _ = r_kinds[kind]
        part = rall_h.at[pl.ds(2 * origin + half[0], half[1])]
        remote(part, part, send_sem.at[kind], recv_sem.at[kind], target).wait_send()

    def left_copy(n, h):
        return remote(left_h.at[h, rows(others[n]), :], left.at[2 * me + h], ls_sem.at[2 * n + h], lr_sem.at[2 * n + h],
                      others[n])

    def regroup(dev):
        a, b = (left[2 * dev + h, TAIL:ROWS, :].astype(jnp.float32) for h in range(2))
        left[2 * dev, TAIL:ROWS, :] = jnp.concatenate([a[:8], b[:8]], axis=0).astype(jnp.bfloat16)
        left[2 * dev + 1, TAIL:ROWS, :] = jnp.concatenate([a[8:], b[8:]], axis=0).astype(jnp.bfloat16)

    def left_landed(n):
        for h in range(2):
            part = left.at[2 * others[n] + h]
            remote(part, part, ls_sem.at[2 * n + h], lr_sem.at[2 * n + h], others[n]).wait_recv()
        regroup(others[n])

    def pair_copy(n):
        return remote(pair_h, wall.at[pl.ds(2 * me, 2)], ws_sem.at[n], wr_sem.at[n], others[n])

    def pair_landed(n):
        part = wall.at[pl.ds(2 * others[n], 2)]
        remote(part, part, ws_sem.at[n], wr_sem.at[n], others[n]).wait_recv()

    def psi_copy(n):
        c, p, slot = lax.div(n, NP), lax.rem(n, NP), lax.rem(n, SLOTS)
        return pltpu.make_async_copy(psi_h.at[:, lax.div(p, 4), lax.rem(p, 4), lanes(c)], sig.at[:, lanes(slot)],
                                     psi_sem.at[slot])

    def vector_out(j):
        return [pltpu.make_async_copy(vec.at[pl.ds(p * ROWS, ROWS), :], kry_h.at[j, :, p // 4, p % 4, :],
                                      out_sem.at[p]) for p in range(NP)]

    def chunk_out(j, c):
        for p in range(NP):
            pltpu.make_async_copy(vec.at[pl.ds(p * ROWS, ROWS), lanes(c)], kry_h.at[j, :, p // 4, p % 4, lanes(c)],
                                  out_sem.at[p]).start()

    def fold(x):
        return jnp.sum(x.reshape(-1, 8, LANES), axis=0)

    def everywhere(x):
        return jnp.broadcast_to(jnp.sum(jnp.sum(x, axis=0, keepdims=True), axis=1, keepdims=True), (8, LANES))

    def exchange_start(par):
        exch[par, me] = mine[...]
        copies = [remote(mine, exch.at[par, me], xs_sem.at[n], xr_sem.at[par, n], others[n]) for n in range(NDEV - 1)]
        for cp in copies:
            cp.start()
        return copies

    def exchange_wait(par, copies):
        for n in range(NDEV - 1):
            remote(mine, exch.at[par, others[n]], xs_sem.at[n], xr_sem.at[par, n], others[n]).wait_recv()
    barrier = pltpu.get_barrier_semaphore()
    for n in range(NDEV - 1):
        pl.semaphore_signal(barrier, inc=1, device_id=(others[n],), device_id_type=MESH)
    slab = [pltpu.make_async_copy(psi_h.at[rows(me), p // 4, p % 4, :], vec.at[pl.ds(p * ROWS, ROWS), :],
                                  slab_sem.at[p]) for p in range(NP)]
    for cp in slab:
        cp.start()
    own = [pltpu.make_async_copy(pair_h, wall.at[pl.ds(2 * me, 2)], own_sem.at[0]),
           pltpu.make_async_copy(left_h.at[:, rows(me), :], left.at[pl.ds(2 * me, 2)], own_sem.at[1])]
    for cp in own:
        cp.start()
    rest = [(h, c, rblk.at[(h * NCH + c) // KG, (h * NCH + c) % KG]) for h in range(2) for c in range(NCH)]
    take = [pltpu.make_async_copy(right_h.at[h, :, lanes(c)], at, rest_sem.at[n]) for n, (h, c, at) in enumerate(rest)]
    place_own = [pltpu.make_async_copy(at, rall_h.at[2 * me + h, :, lanes(c)], rest_sem.at[n])
                 for n, (h, c, at) in enumerate(rest)]
    for cp in take:
        cp.start()
    for n in range(SLOTS):
        psi_copy(n).start()
    zero = jnp.zeros((8, LANES), jnp.float32)
    with jax.named_scope('barrier'):
        pl.semaphore_wait(barrier, NDEV - 1)
    for n, h in ((1, 0), (3, 0), (0, 0), (0, 1)):
        left_copy(n, h).start()
    for cp in slab:
        cp.wait()

    def squares(i, acc):
        at = pl.ds(pl.multiple_of(i * LANES, LANES), LANES)
        for c in range(NCH):
            x = vec[at, c * LANES:(c + 1) * LANES]
            acc = acc + fold(x * x)
        return acc

    mine[...] = jnp.full((8, LANES), jnp.sum(lax.fori_loop(0, SLOTS, squares, zero, unroll=2)))
    copies = exchange_start(1)
    for n in range(NDEV - 1):
        pair_copy(n).start()
    for n, h in ((1, 1), (3, 1), (2, 0), (4, 0), (2, 1), (4, 1)):
        left_copy(n, h).start()

    def r_own(c):
        for kind in (4, 0, 2, 1, 3):
            r_send(c, kind)

    def operators_out(c, carry):
        r_own(c)
        return carry

    lax.fori_loop(0, 5, operators_out, 0)
    for n in (5, 6):
        for h in range(2):
            left_copy(n, h).start()
    lax.fori_loop(5, NCH, operators_out, 0)
    for cp in take:
        cp.wait()
    for cp in place_own:
        cp.start()
    with jax.named_scope('exch0'):
        exchange_wait(1, copies)
        for cp in copies:
            cp.wait_send()
    total = exch[1, 0]
    for d in range(1, NDEV):
        total = total + exch[1, d]
    scale[...] = 1.0 / jnp.sqrt(total * (1.0 / ELEMS))

    def normalise(i, carry):
        at = pl.ds(pl.multiple_of(i * LANES, LANES), LANES)
        for c in range(NCH):
            cs = slice(c * LANES, (c + 1) * LANES)
            vec[at, cs] = vec[at, cs] * scale[0:1, :]
        return carry

    lax.fori_loop(0, SLOTS, normalise, 0, unroll=2)
    for cp in vector_out(0):
        cp.start()

    for n in range(NDEV - 1):
        pair_landed(n)
    for cp in own:
        cp.wait()
    spread = (lax.div(lax.broadcasted_iota(jnp.int32, (256, 16), 0), 16)
              == lax.broadcasted_iota(jnp.int32, (256, 16), 1)).astype(jnp.float32).astype(jnp.bfloat16)
    same = (lax.rem(lax.broadcasted_iota(jnp.int32, (256, 256), 0), 16)
            == lax.rem(lax.broadcasted_iota(jnp.int32, (256, 256), 1), 16))

    def piece(n):
        vbuf[lax.div(n, NP), lax.rem(n, NP)] = (
            sig[:, lanes(lax.rem(n, SLOTS))] * scale[0:1, :]).astype(jnp.bfloat16)

    def opening_pieces(k, carry):
        tall = jnp.dot(spread, wall[k], preferred_element_type=jnp.float32).astype(jnp.bfloat16)
        full = lax.dot_general(tall, spread, (((1,), (1,)), ((), ())), preferred_element_type=jnp.float32)
        kron[k] = jnp.where(same, full, 0.0).astype(jnp.bfloat16)
        for t in range(4):
            n = 4 * k + t
            psi_copy(n).wait()
            piece(n)
            psi_copy(n + SLOTS).start()
        return carry

    with jax.named_scope('convert'):
        lax.fori_loop(0, TERMS, opening_pieces, 0)
    left_landed(0)
    regroup(me)
    first_half = lax.rem(lax.broadcasted_iota(jnp.int32, (256, 256), 0), 16) < 8

    def mix(n, carry):
        kmix[n] = jnp.where(first_half, kron[2 * n].astype(jnp.float32),
                            kron[2 * n + 1].astype(jnp.float32)).astype(jnp.bfloat16)
        return carry

    lax.fori_loop(0, TERMS // 2, mix, 0)
    with jax.named_scope('ownwait'):
        for cp in place_own:
            cp.wait()

    chip = lax.div(me, 2)

    def group(rel):
        return chip + lax.rem(rel, 2) * (1 - 2 * xpos) + lax.div(rel, 2) * (2 - 4 * ypos)

    def place(j, u):
        later = lax.div(j + STEPS - 1, STEPS)
        t = lax.div(u, NCH)
        mid, last = lax.div(t * (3 - t), 2), lax.div(t, 3)
        rel0 = mid * (1 + lax.rem(u + 1, 2)) + last * 3
        c0 = (1 - mid - last) * u + mid * lax.div(u - NCH, 2) + last * (u - 3 * NCH)
        c = later * lax.div(u, NKG) + (1 - later) * c0
        rel = later * lax.rem(u, NKG) + (1 - later) * rel0
        return c, rel, group(rel)

    def fetch_start(j, u, slot):
        c, _, kg = place(j, u)
        pltpu.make_async_copy(rall_h.at[pl.ds(kg * KG, KG), :, lanes(c)], rblk.at[slot], r_sem.at[slot]).start()

    def fetch_wait(slot):
        pltpu.make_async_copy(rall_h.at[pl.ds(0, KG), :, lanes(0)], rblk.at[slot], r_sem.at[slot]).wait()

    def stage_left(j, s, g):
        for i in range(NKG):
            c, _, kg = place(j, NKG * s + i)
            rhs = jnp.concatenate([vbuf[c, 4 * g + t] for t in range(4)], axis=1)
            lhs = left[pl.ds(kg * KG, KG)].reshape(KG * ROWS, BOND)
            o = jnp.dot(lhs, rhs, preferred_element_type=jnp.float32).astype(jnp.bfloat16)
            for t in range(4):
                ubuf[4 * g + t, i * KG * ROWS:(i + 1) * KG * ROWS, :] = o[:, t * LANES:(t + 1) * LANES]

    def stage_pair(j, s):
        for i in range(NKG):
            _, _, kg = place(j, NKG * s + i)

            def columns(row):
                return ubuf[:, row:row + 16, :].reshape(256, LANES)

            for k in range(KG):
                row, at = (i * KG + k) * ROWS, k * LANES
                rhs = jnp.concatenate([columns(row + g * 16) for g in range(TAIL // 16)], axis=1)
                o = jnp.dot(kron[kg * KG + k], rhs, preferred_element_type=jnp.float32).astype(jnp.bfloat16)
                for g in range(TAIL // 16):
                    for q in range(NP):
                        zbuf[i, q * ROWS + g * 16:q * ROWS + (g + 1) * 16, at:at + LANES] = (
                            o[q * 16:(q + 1) * 16, g * LANES:(g + 1) * LANES])
            for n in range(KG // 2):
                row = (i * KG + 2 * n) * ROWS + TAIL
                rhs = jnp.concatenate([columns(row), columns(row + ROWS)], axis=1)
                o = jnp.dot(kmix[kg * (KG // 2) + n], rhs, preferred_element_type=jnp.float32)
                for h in range(2):
                    at = (2 * n + h) * LANES
                    for q in range(NP):
                        half = o[q * 16 + 8 * h:q * 16 + 8 * h + 8]
                        zbuf[i, q * ROWS + TAIL:(q + 1) * ROWS, at:at + LANES] = jnp.concatenate(
                            [half[:, :LANES], half[:, LANES:]], axis=0).astype(jnp.bfloat16)

    def stage_right(blocks, part):
        n0, n1 = NS[part][0] * LANES, NS[part][1] * LANES
        lhs = jnp.concatenate([rblk[slot, k] for _, slot in blocks for k in range(KG)], axis=1)
        rhs = jnp.concatenate([zbuf[i, n0:n1, :] for i, _ in blocks], axis=1)
        sig[:, n0:n1] += lax.dot_general(lhs, rhs, (((1,), (1,)), ((), ())), preferred_element_type=jnp.float32)

    def one_step(j, carry):
        beta_prev, cross = carry

        def r_before(q):
            for at, group in ((NKG, (1, 2)), (2 * NKG, (3, 4)), (5 * NKG, (5, 6))):
                @pl.when(q == at)
                def _(group=group):
                    for n in group:
                        left_landed(n)

            @pl.when((q >= 8) & (q < 8 + 2 * NCH) & (lax.rem(q, 2) == 0))
            def _():
                c = lax.div(q - 8, 2)
                for kind in (0, 2, 1, 3):
                    r_landed(c, kind)
                for kind in (5, 6, 7, 8):
                    r_send(c, kind)

            @pl.when(q >= 22)
            def _():
                c = q - 22
                r_landed(c, 5)
                r_landed(c, 6)
                r_send(c, 9)

        def fetch(u, slot=None):
            @pl.when(j == 0)
            def _():
                @pl.when(u < NCH)
                def _():
                    r_landed(u, 4)

                for odd, kind in ((1, 7), (0, 8)):
                    @pl.when((u >= NCH) & (u < 3 * NCH) & (lax.rem(u, 2) == odd))
                    def _(kind=kind):
                        r_landed(lax.div(u - NCH, 2), kind)

                @pl.when(u >= 3 * NCH)
                def _():
                    r_landed(u - 3 * NCH, 9)

            fetch_start(j, u, lax.rem(u, NKG) if slot is None else slot)

        def opening(g, carry):
            with jax.named_scope('first'):
                near, own = g + 1, g + 3
                relay_xy(lax.div(near, NKG), lax.rem(near, NKG))
                send_own(lax.div(own, NKG), lax.rem(own, NKG))
                relay_diag(0, g)
                arrived(0, g)
            with jax.named_scope('L'):
                stage_left(j, 0, g)
            return carry

        def opening_zero(g, carry):
            each = 12
            for t in range(each):
                psi_copy(4 * NP + each * g + t).wait()
            for t in range(each):
                piece(4 * NP + each * g + t)
            for t in range(each):
                n = 4 * NP + each * g + t + SLOTS

                @pl.when(n < NP * NCH)
                def _():
                    psi_copy(n).start()
            stage_left(j, 0, g)
            return carry

        @pl.when(j == 0)
        def _():
            with jax.named_scope('L0'):
                lax.fori_loop(0, NKG, opening_zero, 0)
                sig[...] = jnp.zeros((BOND, SLAB), jnp.float32)

        @pl.when(j > 0)
        def _():
            relay_xy(0, 0)
            send_own(0, 2)
            lax.fori_loop(0, NKG, opening, 0)
            with jax.named_scope('first3'):
                relay_xy(1, 1)
                send_own(1, 3)
                relay_diag(1, 0)
        for u in range(3):
            fetch(u)
        with jax.named_scope('W'):
            stage_pair(j, 0)

        def chunk(s, carry):
            def unit(g, carry):
                with jax.named_scope('before'):
                    @pl.when(j == 0)
                    def _():
                        r_before(NKG * s + g)

                    @pl.when(j > 0)
                    def _():
                        @pl.when(NKG * s + g < UNITS - 2)
                        def _():
                            ahead = g + 2
                            relay_xy(s + lax.div(ahead, NKG), lax.rem(ahead, NKG))

                        @pl.when(s < NCH - 1)
                        def _():
                            send_own(s + 1, g)

                        relay_diag(s, g + 1)
                        arrived(s, g)
                with jax.named_scope('RL'):
                    fetch_wait(g)
                    stage_left(j, s, g)
                    for part in range(len(NS)):
                        stage_right(((g, g),), part)
                with jax.named_scope('after'):
                    fetch(NKG * s + g - 1)
                return carry

            lax.fori_loop(0, NKG - 1, unit, 0)
            with jax.named_scope('before'):
                @pl.when(j == 0)
                def _():
                    r_before(NKG * s + NKG - 1)

                @pl.when(j > 0)
                def _():
                    @pl.when(s < NCH - 1)
                    def _():
                        relay_diag(s + 1, 0)
                        relay_xy(s + 1, 1)
                        send_own(s + 1, 3)

                    @pl.when(s == NCH - 1)
                    def _():
                        fetch_start(j, UNITS - 2, NKG - 2)
                        fetch_start(j, UNITS - 1, NKG)

                    arrived(s, NKG - 1)
            with jax.named_scope('LRW'):
                fetch_wait(NKG - 1)
                stage_left(j, s, NKG - 1)
                for part in range(len(NS)):
                    stage_right(((NKG - 1, NKG - 1),), part)
                stage_pair(j, s)
            with jax.named_scope('after'):
                @pl.when((j == 0) | (s < NCH - 1))
                def _():
                    fetch(NKG * s + 2)
            return carry

        lax.fori_loop(1, NCH, chunk, 0)

        @pl.when(j == 0)
        def _():
            r_before(UNITS)
            fetch(UNITS - 1, NKG)

        with jax.named_scope('sent'):
            @pl.when(j == 0)
            def _():
                for kind in range(NR):
                    r_sent(kind)
                for n in range(NDEV - 1):
                    for h in range(2):
                        left_copy(n, h).wait_send()
                    pair_copy(n).wait_send()

            @pl.when(j > 0)
            def _():
                for kind in range(len(v_kinds)):
                    v_sent(kind)

        with jax.named_scope('tail'):
            blocks = ((0, 0), (1, 1), (2, 2), (3, NKG))
            for _, slot in blocks:
                fetch_wait(slot)
            b_sum, v_sum = zero, zero
            for part in range(len(NS)):
                stage_right(blocks, part)
                for i in range(*NS[part]):
                    at = slice(i * LANES, (i + 1) * LANES)
                    for c in range(NCH):
                        cs = slice(c * LANES, (c + 1) * LANES)
                        s = sig[cs, at].T
                        v = vec[at, cs]
                        sig[cs, at] = s
                        b_sum = b_sum + fold(s * v)
                        v_sum = v_sum + fold(v * v)

        b_row, v_row = everywhere(b_sum), everywhere(v_sum)
        a_row = b_row + beta_prev * cross
        held = v_row > 1e-20
        fit = jnp.where(held, b_row / jnp.where(held, v_row, 1.0), 0.0)
        fit_row = fit[0:1, :]

        def second(i, n_sum):
            at = pl.ds(pl.multiple_of(i * LANES, LANES), LANES)
            for c in range(NCH):
                cs = slice(c * LANES, (c + 1) * LANES)
                d = sig[cs, at] - fit_row * vec[at, cs]
                n_sum = n_sum + fold(d * d)
            return n_sum

        with jax.named_scope('pass2'):
            n_row = everywhere(lax.fori_loop(0, SLOTS, second, zero, unroll=2))
        for cp in vector_out(j):
            cp.wait()

        row_id = lax.broadcasted_iota(jnp.int32, (8, LANES), 0)
        mine[...] = jnp.where(row_id == 0, a_row, jnp.where(
            row_id == 1, jnp.sqrt(v_row), jnp.where(row_id == 2, fit, n_row)))
        par = lax.rem(j, 2)
        with jax.named_scope('exch'):
            copies = exchange_start(par)
            exchange_wait(par, copies)
        total = exch[par, 0]
        for d in range(1, NDEV):
            total = total + exch[par, d]
        alpha = total[0:1, :] * (1.0 / ELEMS)
        square = jnp.zeros((1, LANES), jnp.float32)
        for d in range(NDEV):
            part = exch[par, d]
            gap = (alpha - part[2:3, :]) * part[1:2, :]
            square = square + (part[3:4, :] + gap * gap)
        beta = jnp.sqrt(square * (1.0 / ELEMS))
        inv = 1.0 / beta
        ab_ref[j] = jnp.concatenate([alpha, beta] + [alpha] * 6, axis=0)

        def third(c, x_sum):
            cs = lanes(c)
            for i in range(SLOTS):
                at = slice(i * LANES, (i + 1) * LANES)
                v = vec[at, cs]
                n = (sig[cs, at] - alpha * v) * inv
                x_sum = x_sum + fold(v * n)
                vec[at, cs] = n
                low = n.astype(jnp.bfloat16)
                for t in range(8):
                    p, a = divmod(8 * i + t, ROWS // 16)
                    vbuf[c, p, pl.ds(pl.multiple_of(me * ROWS + 16 * a, 16), 16), :] = low[16 * t:16 * t + 16]
                sig[cs, at] = (v * -beta).T

            @pl.when((c < 2) & (j < STEPS - 1))
            def _():
                send_own(0, c)

            chunk_out(j + 1, c)
            return x_sum

        with jax.named_scope('pass3'):
            x_sum = lax.fori_loop(0, NCH, third, zero)
        for cp in copies:
            cp.wait_send()
        return beta, everywhere(x_sum)

    lax.fori_loop(0, STEPS, one_step, (jnp.zeros((1, LANES), jnp.float32), zero))
    for cp in vector_out(STEPS):
        cp.wait()


def lanczos(psi, left, pair, right):
    dma = pltpu.SemaphoreType.DMA
    return pl.pallas_call(
        kernel,
        out_shape=(jax.ShapeDtypeStruct((STEPS + 1, ROWS, 4, 4, BOND), jnp.float32),
                   jax.ShapeDtypeStruct((TERMS, BOND, BOND), jnp.bfloat16),
                   jax.ShapeDtypeStruct((STEPS, 8, LANES), jnp.float32)),
        in_specs=[pl.BlockSpec(memory_space=pl.ANY)] * 4,
        out_specs=(pl.BlockSpec(memory_space=pl.ANY), pl.BlockSpec(memory_space=pl.ANY),
                   pl.BlockSpec(memory_space=pltpu.VMEM)),
        scratch_shapes=[
            pltpu.VMEM((NCH, NP, BOND, LANES), jnp.bfloat16),
            pltpu.VMEM((TERMS, ROWS, BOND), jnp.bfloat16),
            pltpu.VMEM((TERMS, 16, 16), jnp.bfloat16),
            pltpu.VMEM((TERMS, 256, 256), jnp.bfloat16),
            pltpu.VMEM((TERMS // 2, 256, 256), jnp.bfloat16),
            pltpu.VMEM((NKG + 1, KG, BOND, LANES), jnp.bfloat16),
            pltpu.VMEM((BOND, SLAB), jnp.float32),
            pltpu.VMEM((NP, TERMS * ROWS, LANES), jnp.bfloat16),
            pltpu.VMEM((NKG, SLAB, KG * LANES), jnp.bfloat16),
            pltpu.VMEM((SLAB, BOND), jnp.float32),
            pltpu.VMEM((8, LANES), jnp.float32),
            pltpu.VMEM((8, LANES), jnp.float32),
            pltpu.VMEM((2, NDEV, 8, LANES), jnp.float32),
            dma((NP,)), dma((SLOTS,)), dma((2,)), dma((2 * NCH,)), dma((14,)), dma((14,)), dma((NDEV - 1,)), dma((NDEV - 1,)),
            dma((NKG + 1,)), dma((NP,)), dma((10,)), dma((UNITS * 4,)), dma((NDEV - 1,)), dma((2, NDEV - 1)),
        ],
        compiler_params=pltpu.CompilerParams(collective_id=0, has_side_effects=True, vmem_limit_bytes=67043328),
    )(psi, left, pair, right)


def solution(mesh):
    def local_run(psi_init, left_env, op_pair, right_env):
        vectors, _, ab = lanczos(psi_init, left_env, op_pair, right_env)
        return vectors, ab[:, 0, 0], ab[:, 1, 0]

    return jax.shard_map(local_run, mesh=mesh, in_specs=(P(), P('terms'), P('terms'), P('terms')),
                         out_specs=(P(None, 'terms'), P(), P()), check_vma=False)
```
